32 devices in a mesh: seq: 8 (over y, x, core), rep: 4 (over z).
Axes of the slice: x: 2, y: 2, z: 4, core: 2. Of those that a mesh axis runs over, the one named last changes fastest.
Arguments:
- queries: bfloat16 [4096, 2048], P(('rep', 'seq')), parts along dimension 0, may hold values from -6 to 6
- keys: bfloat16 [4096, 2048], P(('rep', 'seq')), parts along dimension 0, may hold values from -6 to 6
- values: bfloat16 [4096, 2048], P(('rep', 'seq')), parts along dimension 0, may hold values from -6 to 6
- short_taps: float32 [3, 3, 2048], replicated, may hold values from -3.5 to 3.5
- decay: float32 [2048, 16], replicated, may hold values from 0.00048828125 to 0.1
- residue: float32 [2048, 16], replicated, may hold values from -1.5 to 1.5
- skip: float32 [2048], replicated, may hold values from -3 to 3
- w_out: bfloat16 [2048, 2048], replicated, may hold values from -0.125 to 0.125
Outputs:
- layer_out: bfloat16 [4096, 2048], P(('rep', 'seq')), parts along dimension 0
The draws below stay inside these ranges and needn't reach their ends.
There are 4 independent parts, one for each index of `rep`. The reference program is written for one: setup_inputs(seed, part) draws one part's arguments, and reference() takes and returns one part's arrays. A program takes and returns all parts, laid end to end along the dimension named above; an argument that names none is the same for every part. Nothing has to cross between parts.
All inputs are finite; a program needn't handle non-finite values.
Results may differ from the reference program's by a relative error of at most 0.014.
Values may be sent and summed in bfloat16 or wider, within the bound.
A program may use at most 64 MiB of HBM per device.

```python
import math
import jax
import jax.numpy as jnp
from jax import lax

D = 2048
MODES = 16
SEQLEN = 1024


def levels(stream_key, extent, shards, smallest, top_value):
    level = 1.0
    for axis_at, parts in shards:
        steps = jax.random.uniform(jax.random.fold_in(jax.random.fold_in(stream_key, 6), axis_at), (parts,), jnp.float32, smallest / len(shards), top_value / len(shards))
        level = level * jnp.repeat(jnp.exp(steps), extent[axis_at] // parts).reshape((-1,) + (1,) * (len(extent) - 1 - axis_at))
    return level


def normal_values(key, extent, deviation, bound, split=(), kind=jnp.bfloat16):
    values = jax.random.normal(key, extent, jnp.float32) * deviation
    if len(split) > 0:
        values = levels(key, extent, split, -0.22, 0.18) * values
    return jnp.clip(values, min=-bound, max=bound).astype(kind)


def setup_inputs(seed: int = 0, part: int = 0) -> dict:
    seeds = jax.random.split(jax.random.key(seed), 9)
    part_keys = jax.random.split(jax.random.fold_in(seeds[8], part), 9)
    return {
        "queries": normal_values(part_keys[0], (SEQLEN, D), 1.0, 6.0, ((0, 8),)),
        "keys": normal_values(part_keys[1], (SEQLEN, D), 1.0, 6.0, ((0, 8),)),
        "values": normal_values(part_keys[2], (SEQLEN, D), 1.0, 6.0, ((0, 8),)),
        "short_taps": normal_values(seeds[3], (3, 3, D), 3 ** -0.5, 3.5, (), jnp.float32),
        "decay": jnp.clip(jnp.exp(jax.random.uniform(seeds[4], (D, MODES), jnp.float32, math.log(0.00048828125), math.log(0.1))), 0.00048828125, 0.1),
        "residue": normal_values(seeds[5], (D, MODES), 0.25, 1.5, (), jnp.float32),
        "skip": normal_values(seeds[6], (D,), 0.5, 3.0, (), jnp.float32),
        "w_out": normal_values(seeds[7], (D, D), D ** -0.5, 0.125),
    }


def short_conv(tokens, taps):
    whole = tokens.astype(jnp.float32)
    width = whole.shape[1]
    result = taps[0] * whole
    first = jnp.concatenate([jnp.zeros((1, width), jnp.float32), whole[:-1]], axis=0)
    second = jnp.concatenate([jnp.zeros((2, width), jnp.float32), whole[:-2]], axis=0)
    return result + taps[1] * first + taps[2] * second

def reference(queries, keys, values, short_taps, decay, residue, skip, w_out):
    q_short = short_conv(queries, short_taps[0])
    k_short = short_conv(keys, short_taps[1])
    v_short = short_conv(values, short_taps[2])
    mixed_in = (k_short * v_short).astype(jnp.bfloat16)
    signal = mixed_in.astype(jnp.float32)
    weights = residue * jnp.sqrt(1.0 - jnp.exp(-2.0 * decay))
    length, width = signal.shape
    group = math.gcd(width, 128)
    count = width // group
    grouped = signal.reshape(length, count, group).transpose(1, 0, 2)
    rate_groups = decay.reshape(count, group, decay.shape[1])
    weight_groups = weights.reshape(count, group, decay.shape[1])

    def one_group(items):
        piece, rates, wts = items
        times = jnp.arange(length, dtype=jnp.float32)
        filt = lax.optimization_barrier(jnp.sum(jnp.exp(-times[:, None, None] * rates[None]) * wts[None], axis=2))
        total = 2 * length
        spectrum = jnp.fft.rfft(piece, total, axis=0) * jnp.fft.rfft(filt, total, axis=0)
        return jnp.fft.irfft(spectrum, total, axis=0)[:length]
    convolved = lax.map(one_group, (grouped, rate_groups, weight_groups))
    convolved = convolved.transpose(1, 0, 2).reshape(length, width)
    long_out = (convolved + skip * signal).astype(jnp.bfloat16)
    gated = (q_short * long_out.astype(jnp.float32)).astype(jnp.bfloat16)
    return jnp.dot(gated, w_out, preferred_element_type=jnp.float32).astype(jnp.bfloat16)
```

```python
import functools
import math

import jax
import jax.numpy as jnp
from jax import lax
from jax.experimental import pallas as pl
from jax.experimental.pallas import tpu as pltpu
from jax.sharding import PartitionSpec as P

MESH = pl.DeviceIdType.MESH
F32 = jnp.float32
SUB = 8


def kernel(
    n, width,
    q_hbm, k_hbm, v_hbm, taps_hbm, rates_hbm, residue_hbm, skip_hbm, w_hbm,
    out_ref,
    q_in, k_in, v_in, taps_ref, rates_ref, residue_ref, skip_ref, w_in, tails_out, tails_in, ext, sig, q_short, partial, states,
    carry_table, tap_table, gated, ends, before, totals, earlier, total_out,
    in_sems, w_sem, tail_sems, pair_send, pair_recv, group_send, group_recv,
):
    rows, chans = q_in.shape
    modes = rates_ref.shape[0]
    blocks = rows // SUB
    chunks = chans // width
    groups = n // 2
    me = lax.axis_index("seq")
    group = lax.div(me, 2)
    odd = lax.rem(me, 2)

    barrier = pltpu.get_barrier_semaphore()

    def greet(step, carry):
        pl.semaphore_signal(
            barrier, inc=1, device_id={"seq": lax.rem(me + step, n)}, device_id_type=MESH
        )
        return carry

    lax.fori_loop(1, n, greet, 0)
    loads = [
        pltpu.make_async_copy(src, dst, in_sems.at[i])
        for i, (src, dst) in enumerate((
            (q_hbm, q_in), (k_hbm, k_in), (v_hbm, v_in), (rates_hbm, rates_ref),
            (residue_hbm, residue_ref), (skip_hbm, skip_ref), (taps_hbm, taps_ref),
        ))
    ]
    for load in loads:
        load.start()
    w_load = pltpu.make_async_copy(w_hbm, w_in, w_sem)
    w_load.start()

    for load in loads[:3]:
        load.wait()
    for i, tokens in enumerate((q_in, k_in, v_in)):
        last = tokens[rows - 16 :, :].astype(F32)
        tails_out[2 * i : 2 * i + 2, :] = last[14:16]
    tails_out[6:8, :] = jnp.zeros((2, chans), F32)
    pl.semaphore_wait(barrier, n - 1)

    def tail_copy():
        return pltpu.make_async_remote_copy(
            src_ref=tails_out, dst_ref=tails_in, send_sem=tail_sems.at[0], recv_sem=tail_sems.at[1],
            device_id={"seq": lax.rem(me + 1, n)}, device_id_type=MESH,
        )

    def pair_copy(g):
        return pltpu.make_async_remote_copy(
            src_ref=ends.at[g], dst_ref=before.at[g], send_sem=pair_send.at[g], recv_sem=pair_recv.at[g],
            device_id={"seq": me + 1 - 2 * odd}, device_id_type=MESH,
        )

    def group_copy(source, target, core, g):
        return pltpu.make_async_remote_copy(
            src_ref=totals.at[g], dst_ref=earlier.at[source, g],
            send_sem=group_send.at[target, core, g], recv_sem=group_recv.at[source, g],
            device_id={"seq": 2 * target + core}, device_id_type=MESH,
        )

    @pl.when(me < n - 1)
    def _():
        tail_copy().start()

    @pl.when(me == 0)
    def _():
        tails_in[...] = jnp.zeros_like(tails_in)

    @pl.when(odd == 0)
    def _():
        before[...] = jnp.zeros_like(before)

    for load in loads[3:]:
        load.wait()

    place = lax.broadcasted_iota(jnp.int32, (SUB, width), 0)
    steps = (place + 1).astype(F32)

    def tables(g, carry):
        cols = pl.ds(pl.multiple_of(g * width, width), width)
        rates = rates_ref[:, cols]
        weights = residue_ref[:, cols] * jnp.sqrt(1.0 - jnp.exp(-2.0 * rates))
        total = jnp.zeros((SUB, width), F32)
        for m in range(modes):
            row = jnp.exp(-rates[m : m + 1] * steps) * weights[m : m + 1]
            carry_table[m * SUB : (m + 1) * SUB, cols] = row
            total = total + row
        first = jnp.sum(weights, axis=0, keepdims=True) + skip_ref[:, cols]
        taps = jnp.where(place == 0, first, pltpu.roll(total, 1, 0))
        for s in range(SUB):
            shifted = taps if s == 0 else jnp.where(place >= s, pltpu.roll(taps, s, 0), 0.0)
            tap_table[s * SUB : (s + 1) * SUB, cols] = shifted
        return carry

    lax.fori_loop(0, chunks, tables, 0)

    strip = math.gcd(rows, 16)

    def mix(g, first, last):
        cols = pl.ds(pl.multiple_of(g * width, width), width)
        for i, tokens in enumerate((q_in, k_in, v_in)):
            for r in range(max(first - strip, 0), last, strip):
                ext[i, SUB + r : SUB + r + strip, :] = tokens[r : r + strip, cols].astype(F32)

        def short(i, r):
            result = taps_ref[i, 0:1, cols] * ext[i, SUB + r : SUB + r + strip, :]
            result = result + taps_ref[i, 1:2, cols] * ext[i, SUB + r - 1 : SUB + r + strip - 1, :]
            return result + taps_ref[i, 2:3, cols] * ext[i, SUB + r - 2 : SUB + r + strip - 2, :]

        for r in range(first, last, strip):
            mixed = (short(1, r) * short(2, r)).astype(jnp.bfloat16)
            mixed = mixed.astype(F32)
            for j in range(0, strip, SUB):
                sig[(r + j) // SUB, :, cols] = mixed[j : j + SUB]
            q_short[r : r + strip, cols] = short(0, r)

    def mix_later(g, carry):
        mix(g, strip, rows)
        return carry

    lax.fori_loop(0, chunks, mix_later, 0)

    @pl.when(me > 0)
    def _():
        tail_copy().wait_recv()

    def combine(g):
        @pl.when(odd == 1)
        def _():
            pair_copy(g).wait_recv()

            @pl.when(group < groups - 1)
            def _():
                cols = pl.ds(pl.multiple_of(g * width, width), width)
                span = jnp.exp(-float(rows) * rates_ref[:, cols])
                totals[g] = (span * before[g] + ends[g]).astype(totals.dtype)

                def send(target, carry):
                    for core in range(2):
                        group_copy(group, target, core, g).start()
                    return carry

                lax.fori_loop(group + 1, groups, send, 0)

    def local(g, carry):
        cols = pl.ds(pl.multiple_of(g * width, width), width)
        for i in range(3):
            ext[i, SUB - 2 : SUB, :] = tails_in[2 * i : 2 * i + 2, cols]
        mix(g, 0, strip)
        fade = jnp.exp(-rates_ref[:, cols])

        def block(b, state):
            states[b, :, cols] = state
            base = pl.multiple_of(b * SUB, SUB)
            acc = None
            for s in range(SUB):
                row = sig[b, s : s + 1, cols]
                state = state * fade + row
                term = tap_table[s * SUB : (s + 1) * SUB, cols] * row
                acc = term if acc is None else acc + term
            partial[pl.ds(base, SUB), cols] = acc
            return state

        ends[g] = lax.fori_loop(0, blocks, block, jnp.zeros((modes, width), F32), unroll=2)

        @pl.when(odd == 0)
        def _():
            pair_copy(g).start()

        @pl.when(g > 0)
        def _():
            combine(g - 1)

        return carry

    lax.fori_loop(0, chunks, local, 0)
    combine(chunks - 1)
    w_load.wait()
    batch = 4 if blocks % 4 == 0 else 1
    tile = out_ref.shape[1] // (blocks // batch)

    def project(g, side, k):
        source = pl.ds(pl.multiple_of(g * width, width), width)
        here = pl.ds(pl.multiple_of(k * tile, tile), tile)
        piece = jnp.dot(gated[side], w_in[source, here], preferred_element_type=F32)
        total_out[:, here] += piece

    def finish(g, carry):
        cols = pl.ds(pl.multiple_of(g * width, width), width)
        rates = rates_ref[:, cols]
        far = jnp.exp(-2.0 * rows * rates)

        def gather(source, state):
            group_copy(source, group, odd, g).wait_recv()
            return state * far + earlier[source, g].astype(F32)

        entering = lax.fori_loop(0, group, gather, jnp.zeros((modes, width), F32))
        span = jnp.where(odd == 1, jnp.exp(-float(rows) * rates), 1.0)
        entering = span * entering + before[g]
        fade = jnp.exp(-float(SUB) * rates)
        for b in range(blocks):
            states[b, :, cols] = states[b, :, cols] + entering
            entering = entering * fade

        side = lax.rem(g, 2)

        def outputs(k, inner):
            project(jnp.maximum(g - 1, 0), 1 - side, k)
            base = pl.multiple_of(k * batch * SUB, batch * SUB)
            accs = [partial[pl.ds(base + j * SUB, SUB), cols] for j in range(batch)]
            for m in range(modes):
                table = carry_table[m * SUB : (m + 1) * SUB, cols]
                for j in range(batch):
                    row = states[k * batch + j, m : m + 1, cols]
                    accs[j] = accs[j] + table * row
            long_out = jnp.concatenate(accs, axis=0).astype(jnp.bfloat16).astype(F32)
            here = pl.ds(base, batch * SUB)
            gated[side, here, :] = (q_short[here, cols] * long_out).astype(jnp.bfloat16)
            return inner

        lax.fori_loop(0, blocks // batch, outputs, 0)
        return carry

    gated[1] = jnp.zeros(gated.shape[1:], gated.dtype)
    total_out[...] = jnp.zeros_like(total_out)
    lax.fori_loop(0, chunks, finish, 0)
    for k in range(blocks // batch):
        here = slice(k * tile, (k + 1) * tile)
        piece = jnp.dot(
            gated[(chunks - 1) % 2], w_in[chans - width :, here], preferred_element_type=F32
        )
        out_ref[:, here] = (total_out[:, here] + piece).astype(out_ref.dtype)

    @pl.when(me < n - 1)
    def _():
        tail_copy().wait_send()

    @pl.when(odd == 0)
    def _():
        for g in range(chunks):
            pair_copy(g).wait_send()

    @pl.when(odd == 1)
    def _():
        def sent(target, carry):
            for core in range(2):
                for g in range(chunks):
                    group_copy(group, target, core, g).wait_send()
            return carry

        lax.fori_loop(group + 1, groups, sent, 0)


def solution(mesh):
    n = mesh.shape["seq"]

    def body(queries, keys, values, short_taps, decay, residue, skip, w_out):
        rows, chans = queries.shape
        modes = decay.shape[1]
        width = math.gcd(chans, 512)
        chunks = chans // width
        bf16 = jnp.bfloat16
        vmem = pl.BlockSpec(memory_space=pltpu.VMEM)
        hbm = pl.BlockSpec(memory_space=pl.ANY)
        dma = pltpu.SemaphoreType.DMA
        return pl.pallas_call(
            functools.partial(kernel, n, width),
            out_shape=pltpu.VMEM((rows, w_out.shape[1]), bf16),
            in_specs=[hbm] * 8,
            out_specs=vmem,
            scratch_shapes=[
                pltpu.VMEM((rows, chans), bf16),
                pltpu.VMEM((rows, chans), bf16),
                pltpu.VMEM((rows, chans), bf16),
                pltpu.VMEM(short_taps.shape, F32),
                pltpu.VMEM((modes, chans), F32),
                pltpu.VMEM((modes, chans), F32),
                pltpu.VMEM((1, chans), F32),
                pltpu.VMEM(w_out.shape, bf16),
                pltpu.VMEM((SUB, chans), F32),
                pltpu.VMEM((SUB, chans), F32),
                pltpu.VMEM((3, rows + SUB, width), F32),
                pltpu.VMEM((rows // SUB, SUB, chans), F32),
                pltpu.VMEM((rows, chans), F32),
                pltpu.VMEM((rows, chans), F32),
                pltpu.VMEM((rows // SUB, modes, chans), F32),
                pltpu.VMEM((modes * SUB, chans), F32),
                pltpu.VMEM((SUB * SUB, chans), F32),
                pltpu.VMEM((2, rows, width), bf16),
                pltpu.VMEM((chunks, modes, width), F32),
                pltpu.VMEM((chunks, modes, width), F32),
                pltpu.VMEM((chunks, modes, width), bf16),
                pltpu.VMEM((n // 2, chunks, modes, width), bf16),
                pltpu.VMEM((rows, w_out.shape[1]), F32),
                dma((7,)),
                dma,
                dma((2,)),
                dma((chunks,)),
                dma((chunks,)),
                dma((n // 2, 2, chunks)),
                dma((n // 2, chunks)),
            ],
            compiler_params=pltpu.CompilerParams(
                collective_id=0, has_side_effects=True, vmem_limit_bytes=40 * 1024 * 1024
            ),
        )(*(pltpu.with_memory_space_constraint(x, pltpu.HBM) for x in (queries, keys, values, short_taps, decay.T, residue.T, skip[None, :], w_out)))

    placed = (P(("rep", "seq"), None),) * 3 + (P(),) * 5
    return jax.shard_map(
        body, mesh=mesh, in_specs=placed, out_specs=P(("rep", "seq"), None), check_vma=False
    )
```

```python
import functools
import math

import jax
import jax.numpy as jnp
from jax import lax
from jax.experimental import pallas as pl
from jax.experimental.pallas import tpu as pltpu
from jax.sharding import PartitionSpec as P

MESH = pl.DeviceIdType.MESH
F32 = jnp.float32
BF16 = jnp.bfloat16
SUB = 8
LANES = 128


def kernel(
    n, width,
    q_hbm, k_hbm, v_hbm, taps_hbm, rates_hbm, residue_hbm, skip_hbm, w_hbm,
    out_ref,
    q_in, k_in, v_in, taps_ref, rates_ref, residue_ref, skip_ref, w_in,
    tails_out, tails_in, order, moved, fade_ref, skip2_ref, stride_ref, span_ref, weight_ref,
    filter_ref, edge, sig, q_short, partial, local, segments, turn, natural,
    gated, entry, ends, before, totals, earlier, total_out,
    in_sems, w_sem, tail_sems, pair_send, pair_recv, group_send, group_recv, credits,
):
    rows, chans = q_in.shape
    modes = rates_ref.shape[0]
    steps = rows // SUB
    chunks = chans // width
    cells = width // LANES
    groups = n // 2
    me = lax.axis_index("seq")
    group = lax.div(me, 2)
    odd = lax.rem(me, 2)

    barrier = pltpu.get_barrier_semaphore()

    def greet(device):
        pl.semaphore_signal(barrier, inc=1, device_id={"seq": device}, device_id_type=MESH)

    @pl.when(me > 0)
    def _():
        greet(me - 1)

    @pl.when(odd == 1)
    def _():
        def later(device, carry):
            greet(device)
            return carry

        lax.fori_loop(me + 1, n, later, 0)

    loads = [
        pltpu.make_async_copy(src, dst, in_sems.at[i])
        for i, (src, dst) in enumerate((
            (rates_hbm, rates_ref), (k_hbm, k_in), (v_hbm, v_in), (taps_hbm, taps_ref),
            (residue_hbm, residue_ref), (q_hbm, q_in), (skip_hbm, skip_ref),
        ))
    ]
    for load in loads:
        load.start()
    w_load = pltpu.make_async_copy(w_hbm, w_in, w_sem)
    w_load.start()

    def tail_copy():
        return pltpu.make_async_remote_copy(
            src_ref=tails_out, dst_ref=tails_in, send_sem=tail_sems.at[0], recv_sem=tail_sems.at[1],
            device_id={"seq": lax.rem(me + 1, n)}, device_id_type=MESH,
        )

    def pair_copy(g):
        return pltpu.make_async_remote_copy(
            src_ref=ends.at[g], dst_ref=before.at[g], send_sem=pair_send.at[g], recv_sem=pair_recv.at[g],
            device_id={"seq": me + 1 - 2 * odd}, device_id_type=MESH,
        )

    def group_copy(source, target, core, g):
        return pltpu.make_async_remote_copy(
            src_ref=totals.at[g], dst_ref=earlier.at[source, g],
            send_sem=group_send.at[target, core, g], recv_sem=group_recv.at[source, g],
            device_id={"seq": 2 * target + core}, device_id_type=MESH,
        )

    place = lax.broadcasted_iota(jnp.int32, order.shape, 0)
    token = lax.broadcasted_iota(jnp.int32, order.shape, 1)
    wanted = steps * lax.rem(place, SUB) + lax.div(place, SUB) - 2
    order[...] = jnp.where(token == wanted, 1.0, 0.0).astype(BF16)

    @pl.when(me == 0)
    def _():
        tails_in[...] = jnp.zeros_like(tails_in)

    @pl.when(odd == 0)
    def _():
        before[...] = jnp.zeros_like(before)

    total_out[...] = jnp.zeros_like(total_out)
    natural[...] = jnp.zeros_like(natural)
    lane_row = lax.broadcasted_iota(jnp.int32, (SUB, LANES), 0)
    lane_step = lane_row.astype(F32)

    def columns(c):
        return pl.ds(pl.multiple_of(c * LANES, LANES), LANES)

    def chunk(g):
        return pl.ds(pl.multiple_of(g * width, width), width)

    loads[0].wait()

    def rates_tables(g, carry):
        cols = chunk(g)
        rates = rates_ref[:, cols]
        fade_ref[:, cols] = jnp.exp(-rates)
        skip2_ref[:, cols] = jnp.exp(-float(steps - 2) * rates)
        stride_ref[:, cols] = jnp.exp(-float(steps) * rates)
        span_ref[:, cols] = jnp.exp(-float(rows) * rates)
        return carry

    lax.fori_loop(0, chunks, rates_tables, 0)

    for load in loads[1:4]:
        load.wait()

    def short(x, taps, i):
        result = taps[0] * x[SUB * (i + 2) : SUB * (i + 3)]
        result = result + taps[1] * x[SUB * (i + 1) : SUB * (i + 2)]
        return result + taps[2] * x[SUB * i : SUB * (i + 1)]

    def tap_rows(which, cols):
        return [taps_ref[which, j : j + 1, cols] for j in range(3)]

    wide = min(2, cells) * LANES
    strips = chans // wide

    def strip(c):
        return pl.ds(pl.multiple_of(c * wide, wide), wide)

    def arrange(tokens, c):
        return jnp.dot(order[...], tokens[:, strip(c)], preferred_element_type=F32)

    def rounded(x):
        return x.astype(BF16).astype(F32)

    def mix(c, carry):
        slot = lax.rem(c, 2)
        following = jnp.minimum(c + 1, strips - 1)
        next_k = arrange(k_in, following)
        next_v = arrange(v_in, following)
        for half in range(wide // LANES):
            cols = columns(c * (wide // LANES) + half)
            xk = moved.at[slot, 0, :, half * LANES : (half + 1) * LANES]
            xv = moved.at[slot, 1, :, half * LANES : (half + 1) * LANES]
            k_taps = tap_rows(1, cols)
            v_taps = tap_rows(2, cols)
            for i in range(2):
                edge[i, :, cols] = short(xk, k_taps, i)
                edge[2 + i, :, cols] = short(xv, v_taps, i)
            fades = [fade_ref[m : m + 1, cols] for m in range(modes)]
            state = [None] * modes
            for i in range(2, steps):
                u = rounded(short(xk, k_taps, i) * short(xv, v_taps, i))
                sig[i, :, cols] = u
                for m in range(modes):
                    state[m] = u if i == 2 else state[m] * fades[m] + u
            for m in range(modes):
                local[m * SUB : (m + 1) * SUB, cols] = state[m]
        moved[1 - slot, 0] = next_k
        moved[1 - slot, 1] = next_v
        return carry

    moved[0, 0] = arrange(k_in, 0)
    moved[0, 1] = arrange(v_in, 0)
    first_cells = strips // 3
    lax.fori_loop(0, first_cells, mix, 0)

    loads[5].wait()
    for i, tokens in enumerate((q_in, k_in, v_in)):
        last = tokens[rows - 16 :, :].astype(F32)
        tails_out[2 * i : 2 * i + 2, :] = last[14:16]
    tails_out[6:8, :] = jnp.zeros((2, chans), F32)

    pl.semaphore_wait(barrier, jnp.where(me < n - 1, 1, 0) + group)

    @pl.when(me < n - 1)
    def _():
        tail_copy().start()

    def credit(source, carry):
        pl.semaphore_signal(
            credits.at[group], inc=1, device_id={"seq": 2 * source + 1}, device_id_type=MESH
        )
        return carry

    lax.fori_loop(0, group, credit, 0)

    lax.fori_loop(first_cells, strips, mix, 0)

    loads[4].wait()
    loads[6].wait()

    def residue_tables(g, carry):
        cols = chunk(g)
        weight_ref[:, cols] = residue_ref[:, cols] * jnp.sqrt(1.0 - jnp.exp(-2.0 * rates_ref[:, cols]))
        return carry

    lax.fori_loop(0, chunks, residue_tables, 0)

    @pl.when(me > 0)
    def _():
        tail_copy().wait_recv()

    head = lane_row == 0

    def ends_of(which, cols, zeroth, first):
        taps = tap_rows(which, cols)
        one, two = (
            jnp.where(head, tails_in[2 * which + a : 2 * which + a + 1, cols], 0.0) for a in (1, 0)
        )
        return zeroth + taps[1] * one + taps[2] * two, first + taps[2] * one

    def summarize(c, g, half):
        cols = columns(c)
        k0, k1 = ends_of(1, cols, edge[0, :, cols], edge[1, :, cols])
        v0, v1 = ends_of(2, cols, edge[2, :, cols], edge[3, :, cols])
        u0 = rounded(k0 * v0)
        u1 = rounded(k1 * v1)
        sig[0, :, cols] = u0
        sig[1, :, cols] = u1
        for m in range(modes):
            row = slice(m, m + 1)
            start = fade_ref[row, cols] * u0 + u1
            turn[half, m * SUB : (m + 1) * SUB, :] = (
                local[m * SUB : (m + 1) * SUB, cols] + skip2_ref[row, cols] * start
            )
        scale = weight_ref[:, cols] * fade_ref[:, cols]
        stride = stride_ref[:, cols]
        state = None
        for j in range(SUB):
            part = scale * turn[half, pl.ds(j, modes, stride=SUB), :]
            segments[j, :, cols] = part
            state = part if j == 0 else state * stride + part
        ends[g, :, columns(c - g * cells)] = state

    def summaries(g, carry):
        for c in range(cells):
            summarize(g * cells + c, g, c)

        @pl.when(odd == 0)
        def _():
            pair_copy(g).start()

        return carry

    lax.fori_loop(0, chunks, summaries, 0)

    def direct(c, carry):
        slot = lax.rem(c, 2)
        next_q = arrange(q_in, jnp.minimum(c + 1, strips - 1))
        for half in range(wide // LANES):
            cols = columns(c * (wide // LANES) + half)
            response = [jnp.zeros((SUB, LANES), F32) for _ in range(steps // SUB)]
            for m in range(modes):
                row = slice(m, m + 1)
                rates = rates_ref[row, cols]
                term = jnp.exp(-rates * lane_step) * weight_ref[row, cols]
                for b in range(steps // SUB):
                    response[b] = response[b] + term
                    if b + 1 < steps // SUB:
                        term = term * jnp.exp(-float(SUB) * rates)
            response[0] = response[0] + jnp.where(lane_row == 0, skip_ref[:, cols], 0.0)
            for b in range(steps // SUB):
                filter_ref[half, b * SUB : (b + 1) * SUB, :] = response[b]
            xq = moved.at[slot, 0, :, half * LANES : (half + 1) * LANES]
            q_taps = tap_rows(0, cols)
            q0, q1 = ends_of(0, cols, short(xq, q_taps, 0), short(xq, q_taps, 1))
            taps = [filter_ref[half, i : i + 1, :] for i in range(steps)]
            signal = [sig[i, :, cols] for i in range(steps)]
            for i in range(steps):
                q_short[i, :, cols] = q0 if i == 0 else q1 if i == 1 else short(xq, q_taps, i)
                acc = taps[0] * signal[i]
                for s in range(i):
                    acc = acc + taps[i - s] * signal[s]
                partial[i, :, cols] = acc
        moved[1 - slot, 0] = next_q
        return carry

    moved[0, 0] = arrange(q_in, 0)
    lax.fori_loop(0, strips, direct, 0)

    @pl.when(odd == 1)
    def _():
        def combine(g, carry):
            pair_copy(g).wait_recv()

            @pl.when(group < groups - 1)
            def _():
                totals[g] = (span_ref[:, chunk(g)] * before[g] + ends[g]).astype(totals.dtype)

                def send(target, inner):
                    @pl.when(g == 0)
                    def _():
                        pl.semaphore_wait(credits.at[target], 2)

                    for core in range(2):
                        group_copy(group, target, core, g).start()
                    return inner

                lax.fori_loop(group + 1, groups, send, 0)

            return carry

        lax.fori_loop(0, chunks, combine, 0)

    w_load.wait()
    tile = out_ref.shape[1] // cells

    def gather_gated():
        for k in range(cells):
            gated[:, k * LANES : (k + 1) * LANES] = natural[k].astype(BF16)

    def project(g, k):
        here = slice(k * tile, (k + 1) * tile)
        return jnp.dot(gated[...], w_in[chunk(g), here], preferred_element_type=F32)

    def output(g, k):
        cols = columns(g * cells + k)
        state = entry[:, k * LANES : (k + 1) * LANES]
        stride = stride_ref[:, cols]
        for j in range(SUB):
            turn[k, j * modes : (j + 1) * modes, :] = state
            if j + 1 < SUB:
                state = state * stride + segments[j, :, cols]
        flow = [turn[k, pl.ds(m, SUB, stride=modes), :] for m in range(modes)]
        for i in range(steps):
            terms = list(flow)
            while len(terms) > 1:
                terms = [sum(terms[a : a + 2]) for a in range(0, len(terms), 2)]
            long_out = rounded(partial[i, :, cols] + terms[0])
            natural[k, pl.ds(i, SUB, stride=steps), :] = q_short[i, :, cols] * long_out
            if i + 1 < steps:
                flow = [flow[m] * fade_ref[m : m + 1, cols] for m in range(modes)]

    def finish(g, carry):
        span = span_ref[:, chunk(g)]
        far = span * span

        def gather(source, state):
            group_copy(source, group, odd, g).wait_recv()
            return state * far + earlier[source, g].astype(F32)

        entering = lax.fori_loop(0, group, gather, jnp.zeros((modes, width), F32))
        entry[...] = jnp.where(odd == 1, span, 1.0) * entering + before[g]
        gather_gated()
        for k in range(cells):
            total_out[:, k * tile : (k + 1) * tile] += project(jnp.maximum(g - 1, 0), k)
            output(g, k)
        return carry

    lax.fori_loop(0, chunks, finish, 0)
    gather_gated()
    for k in range(cells):
        here = slice(k * tile, (k + 1) * tile)
        out_ref[:, here] = (total_out[:, here] + project(chunks - 1, k)).astype(out_ref.dtype)

    @pl.when(me < n - 1)
    def _():
        tail_copy().wait_send()

    @pl.when(odd == 0)
    def _():
        for g in range(chunks):
            pair_copy(g).wait_send()

    @pl.when(odd == 1)
    def _():
        def sent(target, carry):
            for core in range(2):
                for g in range(chunks):
                    group_copy(group, target, core, g).wait_send()
            return carry

        lax.fori_loop(group + 1, groups, sent, 0)


def solution(mesh):
    n = mesh.shape["seq"]

    def body(queries, keys, values, short_taps, decay, residue, skip, w_out):
        rows, chans = queries.shape
        modes = decay.shape[1]
        width = math.gcd(chans, 512)
        chunks = chans // width
        steps = rows // SUB
        hbm = pl.BlockSpec(memory_space=pl.ANY)
        dma = pltpu.SemaphoreType.DMA
        table = pltpu.VMEM((modes, chans), F32)
        tokens = pltpu.VMEM((rows, chans), BF16)
        placed = pltpu.VMEM((steps, SUB, chans), F32)
        operands = (queries, keys, values, short_taps, decay.T, residue.T, skip[None, :], w_out)
        return pl.pallas_call(
            functools.partial(kernel, n, width),
            out_shape=pltpu.VMEM((rows, w_out.shape[1]), BF16),
            in_specs=[hbm] * 8,
            out_specs=pl.BlockSpec(memory_space=pltpu.VMEM),
            scratch_shapes=[
                tokens, tokens, tokens,
                pltpu.VMEM(short_taps.shape, F32),
                table, table,
                pltpu.VMEM((1, chans), F32),
                pltpu.VMEM(w_out.shape, BF16),
                pltpu.VMEM((SUB, chans), F32),
                pltpu.VMEM((SUB, chans), F32),
                pltpu.VMEM(((steps + 2) * SUB, rows), BF16),
                pltpu.VMEM((2, 2, (steps + 2) * SUB, min(width, 2 * LANES)), F32),
                table, table, table, table, table,
                pltpu.VMEM((2, steps, LANES), F32),
                pltpu.VMEM((4, SUB, chans), F32),
                placed, placed, placed,
                pltpu.VMEM((modes * SUB, chans), F32),
                pltpu.VMEM((SUB, modes, chans), F32),
                pltpu.VMEM((width // LANES, modes * SUB, LANES), F32),
                pltpu.VMEM((width // LANES, rows, LANES), F32),
                pltpu.VMEM((rows, width), BF16),
                pltpu.VMEM((modes, width), F32),
                pltpu.VMEM((chunks, modes, width), F32),
                pltpu.VMEM((chunks, modes, width), F32),
                pltpu.VMEM((chunks, modes, width), BF16),
                pltpu.VMEM((n // 2, chunks, modes, width), BF16),
                pltpu.VMEM((rows, w_out.shape[1]), F32),
                dma((7,)),
                dma,
                dma((2,)),
                dma((chunks,)),
                dma((chunks,)),
                dma((n // 2, 2, chunks)),
                dma((n // 2, chunks)),
                pltpu.SemaphoreType.REGULAR((n // 2,)),
            ],
            compiler_params=pltpu.CompilerParams(
                collective_id=0, has_side_effects=True, vmem_limit_bytes=44 * 1024 * 1024
            ),
        )(*(pltpu.with_memory_space_constraint(x, pltpu.HBM) for x in operands))

    placed = (P(("rep", "seq"), None),) * 3 + (P(),) * 5
    return jax.shard_map(
        body, mesh=mesh, in_specs=placed, out_specs=P(("rep", "seq"), None), check_vma=False
    )
```

```python
import functools
import math

import jax
import jax.numpy as jnp
from jax import lax
from jax.experimental import pallas as pl
from jax.experimental.pallas import tpu as pltpu
from jax.sharding import PartitionSpec as P

MESH = pl.DeviceIdType.MESH
F32 = jnp.float32
BF16 = jnp.bfloat16
SUB = 8
LANES = 128


def kernel(
    n, width,
    q_hbm, k_hbm, v_hbm, taps_hbm, rates_hbm, residue_hbm, skip_hbm, w_hbm,
    out_ref,
    q_in, k_in, v_in, taps_ref, rates_ref, residue_ref, skip_ref, w_in,
    tails_out, tails_in, order, moved, fresh, fade_ref, skip2_ref, stride_ref, span_ref, weight_ref,
    filter_ref, edge, sig, q_short, partial, local, segments, turn, work, natural,
    gated, entry, ends, before, totals, earlier,
    in_sems, w_sem, tail_sems, pair_send, pair_recv, group_send, group_recv, credits,
):
    rows, chans = q_in.shape
    modes = rates_ref.shape[0]
    steps = rows // SUB
    chunks = chans // width
    cells = width // LANES
    groups = n // 2
    me = lax.axis_index("seq")
    group = lax.div(me, 2)
    odd = lax.rem(me, 2)
    zero = lax.div(me, n)

    barrier = pltpu.get_barrier_semaphore()

    def greet(device):
        pl.semaphore_signal(barrier, inc=1, device_id={"seq": device}, device_id_type=MESH)

    @pl.when(me > 0)
    def _():
        greet(me - 1)

    @pl.when(odd == 1)
    def _():
        def later(device, carry):
            greet(device)
            return carry

        lax.fori_loop(me + 1, n, later, 0)

    loads = [
        pltpu.make_async_copy(src, dst, in_sems.at[i])
        for i, (src, dst) in enumerate((
            (rates_hbm, rates_ref), (k_hbm, k_in), (v_hbm, v_in), (taps_hbm, taps_ref),
            (residue_hbm, residue_ref), (q_hbm, q_in), (skip_hbm, skip_ref),
        ))
    ]
    for load in loads:
        load.start()
    w_load = pltpu.make_async_copy(w_hbm, w_in, w_sem)
    w_load.start()

    def tail_copy():
        return pltpu.make_async_remote_copy(
            src_ref=tails_out, dst_ref=tails_in, send_sem=tail_sems.at[0], recv_sem=tail_sems.at[1],
            device_id={"seq": lax.rem(me + 1, n)}, device_id_type=MESH,
        )

    def pair_copy(g):
        return pltpu.make_async_remote_copy(
            src_ref=ends.at[g], dst_ref=before.at[g], send_sem=pair_send.at[g], recv_sem=pair_recv.at[g],
            device_id={"seq": me + 1 - 2 * odd}, device_id_type=MESH,
        )

    def group_copy(source, target, core, g):
        return pltpu.make_async_remote_copy(
            src_ref=totals.at[g], dst_ref=earlier.at[source, g],
            send_sem=group_send.at[target, core, g], recv_sem=group_recv.at[source, g],
            device_id={"seq": 2 * target + core}, device_id_type=MESH,
        )

    place = lax.broadcasted_iota(jnp.int32, order.shape, 0)
    token = lax.broadcasted_iota(jnp.int32, order.shape, 1)
    wanted = steps * lax.rem(place, SUB) + lax.div(place, SUB) - 2
    order[...] = jnp.where(token == wanted, 1.0, 0.0).astype(BF16)

    @pl.when(me == 0)
    def _():
        tails_in[...] = jnp.zeros_like(tails_in)

    @pl.when(odd == 0)
    def _():
        before[...] = jnp.zeros_like(before)

    lane_row = lax.broadcasted_iota(jnp.int32, (SUB, LANES), 0)
    lane_step = lane_row.astype(F32)

    def columns(c):
        return pl.ds(pl.multiple_of(c * LANES, LANES), LANES)

    def chunk(g):
        return pl.ds(pl.multiple_of(g * width, width), width)

    loads[0].wait()

    def rates_tables(g, carry):
        cols = chunk(g)
        rates = rates_ref[:, cols]
        fade_ref[:, cols] = jnp.exp(-rates)
        skip2_ref[:, cols] = jnp.exp(-float(steps - 2) * rates)
        stride_ref[:, cols] = jnp.exp(-float(steps) * rates)
        span_ref[:, cols] = jnp.exp(-float(rows) * rates)
        return carry

    lax.fori_loop(0, chunks, rates_tables, 0)

    for load in loads[1:4]:
        load.wait()

    def short(x, taps, i):
        result = taps[0] * x[SUB * (i + 2) : SUB * (i + 3)]
        result = result + taps[1] * x[SUB * (i + 1) : SUB * (i + 2)]
        return result + taps[2] * x[SUB * i : SUB * (i + 1)]

    def tap_rows(which, cols):
        return [taps_ref[which, j : j + 1, cols] for j in range(3)]

    wide = min(2, cells) * LANES
    strips = chans // wide

    def strip(c):
        return pl.ds(pl.multiple_of(c * wide, wide), wide)

    def arrange(tokens, c):
        return jnp.dot(order[...], tokens[:, strip(c)], preferred_element_type=F32)

    def rounded(x):
        return x.astype(BF16).astype(F32)

    def mix(c, carry):
        following = jnp.minimum(c + 1, strips - 1)
        moved[:2] = fresh[...]
        fresh[0] = arrange(k_in, following)
        fresh[1] = arrange(v_in, following)
        for half in range(wide // LANES):
            cols = columns(c * (wide // LANES) + half)
            xk = moved.at[0, :, half * LANES : (half + 1) * LANES]
            xv = moved.at[1, :, half * LANES : (half + 1) * LANES]
            k_taps = tap_rows(1, cols)
            v_taps = tap_rows(2, cols)
            for i in range(2):
                edge[i, :, cols] = short(xk, k_taps, i)
                edge[2 + i, :, cols] = short(xv, v_taps, i)
            fades = [fade_ref[m : m + 1, cols] for m in range(modes)]
            state = [None] * modes
            for i in range(2, steps):
                u = rounded(short(xk, k_taps, i) * short(xv, v_taps, i))
                sig[i, :, cols] = u
                for m in range(modes):
                    state[m] = u if i == 2 else state[m] * fades[m] + u
            for m in range(modes):
                local[m * SUB : (m + 1) * SUB, cols] = state[m]
            for m in range(0, modes, 4):
                moved[zero + 2, m // 4 * SUB : (m // 4 + 1) * SUB, :LANES] = state[m + 3]
        return carry

    fresh[0] = arrange(k_in, 0)
    fresh[1] = arrange(v_in, 0)
    first_cells = strips // 3
    lax.fori_loop(0, first_cells, mix, 0)

    loads[5].wait()
    for i, tokens in enumerate((q_in, k_in, v_in)):
        last = tokens[rows - 16 :, :].astype(F32)
        tails_out[2 * i : 2 * i + 2, :] = last[14:16]
    tails_out[6:8, :] = jnp.zeros((2, chans), F32)

    pl.semaphore_wait(barrier, jnp.where(me < n - 1, 1, 0) + group)

    @pl.when(me < n - 1)
    def _():
        tail_copy().start()

    def credit(source, carry):
        pl.semaphore_signal(
            credits.at[group], inc=1, device_id={"seq": 2 * source + 1}, device_id_type=MESH
        )
        return carry

    lax.fori_loop(0, group, credit, 0)

    lax.fori_loop(first_cells, strips, mix, 0)

    loads[4].wait()
    loads[6].wait()

    def residue_tables(g, carry):
        cols = chunk(g)
        weight_ref[:, cols] = residue_ref[:, cols] * jnp.sqrt(1.0 - jnp.exp(-2.0 * rates_ref[:, cols]))
        return carry

    lax.fori_loop(0, chunks, residue_tables, 0)

    @pl.when(me > 0)
    def _():
        tail_copy().wait_recv()

    head = lane_row == 0

    def ends_of(which, cols, zeroth, first):
        taps = tap_rows(which, cols)
        one, two = (
            jnp.where(head, tails_in[2 * which + a : 2 * which + a + 1, cols], 0.0) for a in (1, 0)
        )
        return zeroth + taps[1] * one + taps[2] * two, first + taps[2] * one

    def summarize(c, g, half):
        cols = columns(c)
        k0, k1 = ends_of(1, cols, edge[0, :, cols], edge[1, :, cols])
        v0, v1 = ends_of(2, cols, edge[2, :, cols], edge[3, :, cols])
        u0 = rounded(k0 * v0)
        u1 = rounded(k1 * v1)
        sig[0, :, cols] = u0
        sig[1, :, cols] = u1
        for m in range(modes):
            row = slice(m, m + 1)
            start = fade_ref[row, cols] * u0 + u1
            turn[half, m * SUB : (m + 1) * SUB, :] = (
                local[m * SUB : (m + 1) * SUB, cols] + skip2_ref[row, cols] * start
            )
        scale = weight_ref[:, cols] * fade_ref[:, cols]
        stride = stride_ref[:, cols]
        state = None
        for j in range(SUB):
            part = scale * turn[half, pl.ds(j, modes, stride=SUB), :]
            segments[j, :, cols] = part
            state = part if j == 0 else state * stride + part
        ends[g, :, columns(c - g * cells)] = state

    def summaries(g, carry):
        for c in range(cells):
            summarize(g * cells + c, g, c)

        @pl.when(odd == 0)
        def _():
            pair_copy(g).start()

        return carry

    lax.fori_loop(0, chunks, summaries, 0)

    def combine(g):
        pair_copy(g).wait_recv()

        @pl.when(group < groups - 1)
        def _():
            totals[g] = (span_ref[:, chunk(g)] * before[g] + ends[g]).astype(totals.dtype)

            def send(target, inner):
                @pl.when(g == 0)
                def _():
                    pl.semaphore_wait(credits.at[target], 2)

                for core in range(2):
                    group_copy(group, target, core, g).start()
                return inner

            lax.fori_loop(group + 1, groups, send, 0)

    def direct(c, carry):
        moved[0] = fresh[0]
        fresh[0] = arrange(q_in, jnp.minimum(c + 1, strips - 1))
        for half in range(wide // LANES):
            cols = columns(c * (wide // LANES) + half)
            response = [jnp.zeros((SUB, LANES), F32) for _ in range(steps // SUB)]
            for m in range(modes):
                row = slice(m, m + 1)
                rates = rates_ref[row, cols]
                term = jnp.exp(-rates * lane_step) * weight_ref[row, cols]
                for b in range(steps // SUB):
                    response[b] = response[b] + term
                    if b + 1 < steps // SUB:
                        term = term * jnp.exp(-float(SUB) * rates)
            response[0] = response[0] + jnp.where(lane_row == 0, skip_ref[:, cols], 0.0)
            for b in range(steps // SUB):
                filter_ref[half, b * SUB : (b + 1) * SUB, :] = response[b]
            xq = moved.at[0, :, half * LANES : (half + 1) * LANES]
            q_taps = tap_rows(0, cols)
            q0, q1 = ends_of(0, cols, short(xq, q_taps, 0), short(xq, q_taps, 1))
            taps = [filter_ref[half, i : i + 1, :] for i in range(steps)]
            signal = [sig[i, :, cols] for i in range(steps)]
            for i in range(steps):
                q_short[i, :, cols] = q0 if i == 0 else q1 if i == 1 else short(xq, q_taps, i)
                acc = taps[0] * signal[i]
                for s in range(i):
                    acc = acc + taps[i - s] * signal[s]
                partial[i, :, cols] = acc
        return carry

    fresh[0] = arrange(q_in, 0)
    lead = strips // 2
    lax.fori_loop(0, lead, direct, 0)

    def combine_and_direct(g, carry):
        @pl.when(odd == 1)
        def _():
            combine(g)

        return lax.fori_loop(lead + g * (strips - lead) // chunks, lead + (g + 1) * (strips - lead) // chunks, direct, carry)

    lax.fori_loop(0, chunks, combine_and_direct, 0)

    def enter(g, k):
        cols = columns(g * cells + k)
        state = entry[:, k * LANES : (k + 1) * LANES]
        stride = stride_ref[:, cols]
        for j in range(SUB):
            work[k, j * modes : (j + 1) * modes, :] = state
            if j + 1 < SUB:
                state = state * stride + segments[j, :, cols]

    def output(g, k):
        cols = columns(g * cells + k)
        flow = [work[k, pl.ds(m, SUB, stride=modes), :] for m in range(modes)]
        fades = [fade_ref[m : m + 1, cols] for m in range(modes)]
        for i in range(steps):
            terms = list(flow)
            while len(terms) > 1:
                terms = [sum(terms[a : a + 2]) for a in range(0, len(terms), 2)]
            long_out = rounded(partial[i, :, cols] + terms[0])
            natural[pl.ds(i, SUB, stride=steps), :] = q_short[i, :, cols] * long_out
            if i + 1 < steps:
                flow = [flow[m] * fades[m] for m in range(modes)]
        gated[g * cells + k] = natural[...].astype(BF16)

    def finish(g, carry):
        span = span_ref[:, chunk(g)]
        far = span * span

        def gather(source, state):
            group_copy(source, group, odd, g).wait_recv()
            return state * far + earlier[source, g].astype(F32)

        entering = lax.fori_loop(0, group, gather, jnp.zeros((modes, width), F32))
        entry[...] = jnp.where(odd == 1, span, 1.0) * entering + before[g]
        for k in range(cells):
            enter(g, k)

        def one(k, inner):
            output(g, k)
            return inner

        lax.fori_loop(0, cells, one, 0)
        return carry

    lax.fori_loop(0, chunks, finish, 0)
    w_load.wait()
    rows_in = jnp.concatenate([gated[c] for c in range(chans // LANES)], axis=1)
    for a in range(0, out_ref.shape[1], 2 * LANES):
        piece = jnp.dot(rows_in, w_in[:, a : a + 2 * LANES], preferred_element_type=F32)
        out_ref[:, a : a + 2 * LANES] = piece.astype(out_ref.dtype)

    @pl.when(me < n - 1)
    def _():
        tail_copy().wait_send()

    @pl.when(odd == 0)
    def _():
        for g in range(chunks):
            pair_copy(g).wait_send()

    @pl.when(odd == 1)
    def _():
        def sent(target, carry):
            for core in range(2):
                for g in range(chunks):
                    group_copy(group, target, core, g).wait_send()
            return carry

        lax.fori_loop(group + 1, groups, sent, 0)


def solution(mesh):
    n = mesh.shape["seq"]

    def body(queries, keys, values, short_taps, decay, residue, skip, w_out):
        rows, chans = queries.shape
        modes = decay.shape[1]
        width = math.gcd(chans, 512)
        chunks = chans // width
        steps = rows // SUB
        hbm = pl.BlockSpec(memory_space=pl.ANY)
        dma = pltpu.SemaphoreType.DMA
        table = pltpu.VMEM((modes, chans), F32)
        tokens = pltpu.VMEM((rows, chans), BF16)
        placed = pltpu.VMEM((steps, SUB, chans), F32)
        operands = (queries, keys, values, short_taps, decay.T, residue.T, skip[None, :], w_out)
        return pl.pallas_call(
            functools.partial(kernel, n, width),
            out_shape=pltpu.VMEM((rows, w_out.shape[1]), BF16),
            in_specs=[hbm] * 8,
            out_specs=pl.BlockSpec(memory_space=pltpu.VMEM),
            scratch_shapes=[
                tokens, tokens, tokens,
                pltpu.VMEM(short_taps.shape, F32),
                table, table,
                pltpu.VMEM((1, chans), F32),
                pltpu.VMEM(w_out.shape, BF16),
                pltpu.VMEM((SUB, chans), F32),
                pltpu.VMEM((SUB, chans), F32),
                pltpu.VMEM(((steps + 2) * SUB, rows), BF16),
                pltpu.VMEM((3, (steps + 2) * SUB, min(width, 2 * LANES)), F32),
                pltpu.VMEM((2, (steps + 2) * SUB, min(width, 2 * LANES)), F32),
                table, table, table, table, table,
                pltpu.VMEM((2, steps, LANES), F32),
                pltpu.VMEM((4, SUB, chans), F32),
                placed, placed, placed,
                pltpu.VMEM((modes * SUB, chans), F32),
                pltpu.VMEM((SUB, modes, chans), F32),
                pltpu.VMEM((width // LANES, modes * SUB, LANES), F32),
                pltpu.VMEM((width // LANES, modes * SUB, LANES), F32),
                pltpu.VMEM((rows, LANES), F32),
                pltpu.VMEM((chans // LANES, rows, LANES), BF16),
                pltpu.VMEM((modes, width), F32),
                pltpu.VMEM((chunks, modes, width), F32),
                pltpu.VMEM((chunks, modes, width), F32),
                pltpu.VMEM((chunks, modes, width), BF16),
                pltpu.VMEM((n // 2, chunks, modes, width), BF16),
                dma((7,)),
                dma,
                dma((2,)),
                dma((chunks,)),
                dma((chunks,)),
                dma((n // 2, 2, chunks)),
                dma((n // 2, chunks)),
                pltpu.SemaphoreType.REGULAR((n // 2,)),
            ],
            compiler_params=pltpu.CompilerParams(
                collective_id=0, has_side_effects=True, vmem_limit_bytes=44 * 1024 * 1024
            ),
        )(*(pltpu.with_memory_space_constraint(x, pltpu.HBM) for x in operands))

    placed = (P(("rep", "seq"), None),) * 3 + (P(),) * 5
    return jax.shard_map(
        body, mesh=mesh, in_specs=placed, out_specs=P(("rep", "seq"), None), check_vma=False
    )
```

```python
import functools
import math

import jax
import jax.numpy as jnp
from jax import lax
from jax.experimental import pallas as pl
from jax.experimental.pallas import tpu as pltpu
from jax.sharding import PartitionSpec as P

MESH = pl.DeviceIdType.MESH
F32 = jnp.float32
BF16 = jnp.bfloat16
SUB = 8
LANES = 128


def kernel(
    n, width,
    q_hbm, k_hbm, v_hbm, taps_hbm, rates_hbm, residue_hbm, skip_hbm, w_hbm,
    out_ref,
    q_in, k_in, v_in, taps_ref, rates_ref, residue_ref, skip_ref, w_in,
    tails_out, tails_in, tails, order, moved, fresh, fade_ref, skip2_ref, stride_ref, span_ref, weight_ref,
    filter_ref, edge, sig, q_short, partial, local, segments, turn, work, natural,
    gated, entry, entries, shared, ends, other, totals, earlier,
    in_sems, w_sem, tail_sems, pair_send, pair_recv, group_send, group_recv, share_send, share_recv, credits,
):
    rows, chans = q_in.shape
    modes = rates_ref.shape[0]
    steps = rows // SUB
    chunks = chans // width
    cells = width // LANES
    groups = n // 2
    me = lax.axis_index("seq")
    group = lax.div(me, 2)
    odd = lax.rem(me, 2)
    zero = lax.div(me, n)

    barrier = pltpu.get_barrier_semaphore()

    def greet(device):
        pl.semaphore_signal(barrier, inc=1, device_id={"seq": device}, device_id_type=MESH)

    @pl.when(me > 0)
    def _():
        greet(me - 1)

    def later(target, carry):
        greet(2 * target + odd)
        return carry

    lax.fori_loop(group + 1, groups, later, 0)

    loads = [
        pltpu.make_async_copy(src, dst, in_sems.at[i])
        for i, (src, dst) in enumerate((
            (rates_hbm, rates_ref), (k_hbm, k_in), (v_hbm, v_in), (taps_hbm, taps_ref),
            (residue_hbm, residue_ref), (q_hbm, q_in), (skip_hbm, skip_ref),
        ))
    ]
    for load in loads:
        load.start()
    w_load = pltpu.make_async_copy(w_hbm, w_in, w_sem)

    def tail_copy():
        return pltpu.make_async_remote_copy(
            src_ref=tails_out, dst_ref=tails_in, send_sem=tail_sems.at[0], recv_sem=tail_sems.at[1],
            device_id={"seq": lax.rem(me + 1, n)}, device_id_type=MESH,
        )

    def pair_copy(g):
        return pltpu.make_async_remote_copy(
            src_ref=ends.at[g], dst_ref=other.at[g], send_sem=pair_send.at[g], recv_sem=pair_recv.at[g],
            device_id={"seq": me + 1 - 2 * odd}, device_id_type=MESH,
        )

    def keeper(g):
        return lax.div(2 * g, chunks)

    def group_copy(source, target, g):
        return pltpu.make_async_remote_copy(
            src_ref=totals.at[g], dst_ref=earlier.at[source, g],
            send_sem=group_send.at[target, g], recv_sem=group_recv.at[source, g],
            device_id={"seq": 2 * target + odd}, device_id_type=MESH,
        )

    def share_copy(g):
        return pltpu.make_async_remote_copy(
            src_ref=entries.at[g], dst_ref=shared.at[g], send_sem=share_send.at[g], recv_sem=share_recv.at[g],
            device_id={"seq": me + 1 - 2 * odd}, device_id_type=MESH,
        )

    place = lax.broadcasted_iota(jnp.int32, order.shape, 0)
    token = lax.broadcasted_iota(jnp.int32, order.shape, 1)
    wanted = steps * lax.rem(place, SUB) + lax.div(place, SUB) - 2
    order[...] = jnp.where(token == wanted, 1.0, 0.0).astype(BF16)

    @pl.when(me == 0)
    def _():
        tails_in[...] = jnp.zeros_like(tails_in)

    half = (chunks + 1) // 2

    @pl.when(odd == 0)
    def _():
        for g in range(half, chunks):
            other[g] = jnp.zeros(other.shape[1:], F32)

    @pl.when(group == 0)
    def _():
        shared[...] = jnp.zeros_like(shared)

    lane_row = lax.broadcasted_iota(jnp.int32, (SUB, LANES), 0)
    lane_step = lane_row.astype(F32)

    def columns(c):
        return pl.ds(pl.multiple_of(c * LANES, LANES), LANES)

    def chunk(g):
        return pl.ds(pl.multiple_of(g * width, width), width)

    loads[0].wait()

    def rates_tables(g, carry):
        cols = chunk(g)
        rates = rates_ref[:, cols]
        fade_ref[:, cols] = jnp.exp(-rates)
        skip2_ref[:, cols] = jnp.exp(-float(steps - 2) * rates)
        stride_ref[:, cols] = jnp.exp(-float(steps) * rates)
        span_ref[:, cols] = jnp.exp(-float(rows) * rates)
        return carry

    lax.fori_loop(0, chunks, rates_tables, 0)

    for load in loads[1:4]:
        load.wait()

    loads[5].wait()
    w_load.start()
    last = [tokens[rows - 16 :, :].astype(F32)[14:16] for tokens in (q_in, k_in, v_in)]
    tails_out[...] = jnp.concatenate(last + [jnp.zeros((2, chans), F32)], axis=0).astype(BF16)

    pl.semaphore_wait(barrier, jnp.where(me < n - 1, 1, 0) + group)

    @pl.when(me < n - 1)
    def _():
        tail_copy().start()

    def credit(source, carry):
        pl.semaphore_signal(
            credits.at[group], inc=1, device_id={"seq": 2 * source + odd}, device_id_type=MESH
        )
        return carry

    lax.fori_loop(0, group, credit, 0)

    def short(x, taps, i):
        result = taps[0] * x[SUB * (i + 2) : SUB * (i + 3)]
        result = result + taps[1] * x[SUB * (i + 1) : SUB * (i + 2)]
        return result + taps[2] * x[SUB * i : SUB * (i + 1)]

    def tap_rows(which, cols):
        return [taps_ref[which, j : j + 1, cols] for j in range(3)]

    wide = min(2, cells) * LANES
    strips = chans // wide

    def strip(c):
        return pl.ds(pl.multiple_of(c * wide, wide), wide)

    def arrange(tokens, c):
        return jnp.dot(order[...], tokens[:, strip(c)], preferred_element_type=F32)

    def rounded(x):
        return x.astype(BF16).astype(F32)

    def mix(c, carry):
        following = lax.rem(c + 1, strips)
        moved[:2] = fresh[...]
        fresh[0] = arrange(k_in, following)
        fresh[1] = arrange(v_in, following)
        for half in range(wide // LANES):
            cols = columns(c * (wide // LANES) + half)
            xk = moved.at[0, :, half * LANES : (half + 1) * LANES]
            xv = moved.at[1, :, half * LANES : (half + 1) * LANES]
            k_taps = tap_rows(1, cols)
            v_taps = tap_rows(2, cols)
            for i in range(2):
                edge[i, :, cols] = short(xk, k_taps, i)
                edge[2 + i, :, cols] = short(xv, v_taps, i)
            fades = [fade_ref[m : m + 1, cols] for m in range(modes)]
            state = [None] * modes
            for i in range(2, steps):
                u = rounded(short(xk, k_taps, i) * short(xv, v_taps, i))
                sig[i, :, cols] = u
                for m in range(modes):
                    state[m] = u if i == 2 else state[m] * fades[m] + u
            for m in range(modes):
                local[m * SUB : (m + 1) * SUB, cols] = state[m]
            for m in range(0, modes, 4):
                moved[zero + 2, m // 4 * SUB : (m // 4 + 1) * SUB, :LANES] = state[m + 3]
        return carry

    opening = (1 - odd) * half * (strips // chunks)
    fresh[0] = arrange(k_in, opening)
    fresh[1] = arrange(v_in, opening)
    loads[4].wait()
    loads[6].wait()

    def residue_tables(g, carry):
        cols = chunk(g)
        weight_ref[:, cols] = residue_ref[:, cols] * jnp.sqrt(1.0 - jnp.exp(-2.0 * rates_ref[:, cols]))
        return carry

    lax.fori_loop(0, chunks, residue_tables, 0)

    head = lane_row == 0

    def ends_of(which, cols, zeroth, first):
        taps = tap_rows(which, cols)
        one, two = (
            jnp.where(head, tails[2 * which + a : 2 * which + a + 1, cols], 0.0) for a in (1, 0)
        )
        return zeroth + taps[1] * one + taps[2] * two, first + taps[2] * one

    def summarize(c, g, half):
        cols = columns(c)
        k0, k1 = ends_of(1, cols, edge[0, :, cols], edge[1, :, cols])
        v0, v1 = ends_of(2, cols, edge[2, :, cols], edge[3, :, cols])
        u0 = rounded(k0 * v0)
        u1 = rounded(k1 * v1)
        sig[0, :, cols] = u0
        sig[1, :, cols] = u1
        for m in range(modes):
            row = slice(m, m + 1)
            start = fade_ref[row, cols] * u0 + u1
            turn[half, m * SUB : (m + 1) * SUB, :] = (
                local[m * SUB : (m + 1) * SUB, cols] + skip2_ref[row, cols] * start
            )
        scale = weight_ref[:, cols] * fade_ref[:, cols]
        stride = stride_ref[:, cols]
        state = None
        for j in range(SUB):
            part = scale * turn[half, pl.ds(j, modes, stride=SUB), :]
            segments[j, :, cols] = part
            state = part if j == 0 else state * stride + part
        ends[g, :, columns(c - g * cells)] = state

    def combine(g):
        pair_copy(g).wait_recv()

        @pl.when(group < groups - 1)
        def _():
            mine, theirs = ends[g], other[g]
            former = jnp.where(odd == 1, theirs, mine)
            latter = jnp.where(odd == 1, mine, theirs)
            totals[g] = (span_ref[:, chunk(g)] * former + latter).astype(totals.dtype)

            def send(target, inner):
                @pl.when(lax.rem(g, half) == 0)
                def _():
                    pl.semaphore_wait(credits.at[target], 1)

                group_copy(group, target, g).start()
                return inner

            lax.fori_loop(group + 1, groups, send, 0)

    early = jnp.logical_or(me == 0, odd == 1)
    share = strips // chunks

    def stage(t, carry):
        mixing = jnp.where(early, lax.rem(t, 2) == 0, t < chunks)
        turn_at = jnp.where(early, lax.div(t, 2), lax.rem(t, chunks))
        g = lax.rem(turn_at + (1 - odd) * half, chunks)
        own = keeper(g) == odd

        @pl.when(mixing)
        def _():
            lax.fori_loop(g * share, (g + 1) * share, mix, 0)

        @pl.when(jnp.logical_not(mixing))
        def _():
            @pl.when(turn_at == 0)
            def _():
                @pl.when(me > 0)
                def _():
                    tail_copy().wait_recv()

                tails[...] = tails_in[...].astype(F32)

            for c in range(cells):
                summarize(g * cells + c, g, c)

            @pl.when(jnp.logical_or(odd == 0, jnp.logical_not(own)))
            def _():
                pair_copy(g).start()

            @pl.when(jnp.logical_and(own, jnp.logical_or(odd == 0, me == 1)))
            def _():
                combine(g)

        return carry

    lax.fori_loop(0, 2 * chunks, stage, 0)

    def direct(c, carry):
        moved[0] = fresh[0]
        fresh[0] = arrange(q_in, jnp.minimum(c + 1, strips - 1))
        for half in range(wide // LANES):
            cols = columns(c * (wide // LANES) + half)
            response = [jnp.zeros((SUB, LANES), F32) for _ in range(steps // SUB)]
            for m in range(modes):
                row = slice(m, m + 1)
                rates = rates_ref[row, cols]
                term = jnp.exp(-rates * lane_step) * weight_ref[row, cols]
                for b in range(steps // SUB):
                    response[b] = response[b] + term
                    if b + 1 < steps // SUB:
                        term = term * jnp.exp(-float(SUB) * rates)
            response[0] = response[0] + jnp.where(lane_row == 0, skip_ref[:, cols], 0.0)
            for b in range(steps // SUB):
                filter_ref[half, b * SUB : (b + 1) * SUB, :] = response[b]
            xq = moved.at[0, :, half * LANES : (half + 1) * LANES]
            q_taps = tap_rows(0, cols)
            q0, q1 = ends_of(0, cols, short(xq, q_taps, 0), short(xq, q_taps, 1))
            taps = [filter_ref[half, i : i + 1, :] for i in range(steps)]
            signal = [sig[i, :, cols] for i in range(steps)]
            for i in range(steps):
                q_short[i, :, cols] = q0 if i == 0 else q1 if i == 1 else short(xq, q_taps, i)
                acc = taps[0] * signal[i]
                for s in range(i):
                    acc = acc + taps[i - s] * signal[s]
                partial[i, :, cols] = acc
        return carry

    fresh[0] = arrange(q_in, 0)
    lead = strips // 4
    lax.fori_loop(0, lead, direct, 0)

    def combine_and_direct(g, carry):
        @pl.when(jnp.logical_and(odd == 1, me > 1))
        def _():
            combine(g)

        done = lead + (g - half) * (strips - lead) // (chunks - half)
        upto = lead + (g + 1 - half) * (strips - lead) // (chunks - half)
        return lax.fori_loop(done, upto, direct, carry)

    lax.fori_loop(half, chunks, combine_and_direct, 0)

    def enter(g, k):
        cols = columns(g * cells + k)
        state = entry[:, k * LANES : (k + 1) * LANES]
        stride = stride_ref[:, cols]
        for j in range(SUB):
            work[k, j * modes : (j + 1) * modes, :] = state
            if j + 1 < SUB:
                state = state * stride + segments[j, :, cols]

    def output(g, k):
        cols = columns(g * cells + k)
        flow = [work[k, pl.ds(m, SUB, stride=modes), :] for m in range(modes)]
        fades = [fade_ref[m : m + 1, cols] for m in range(modes)]
        for i in range(steps):
            terms = list(flow)
            while len(terms) > 1:
                terms = [sum(terms[a : a + 2]) for a in range(0, len(terms), 2)]
            long_out = rounded(partial[i, :, cols] + terms[0])
            natural[g * cells + k, pl.ds(i, SUB, stride=steps), :] = q_short[i, :, cols] * long_out
            if i + 1 < steps:
                flow = [flow[m] * fades[m] for m in range(modes)]

    def finish(s, carry):
        g = lax.rem(s + odd * half, chunks)
        own = keeper(g) == odd
        span = span_ref[:, chunk(g)]
        far = span * span
        reach = jnp.where(odd == 1, span, 1.0)

        @pl.when(own)
        def _():
            def gather(source, state):
                group_copy(source, group, g).wait_recv()
                return state * far + earlier[source, g].astype(F32)

            entering = lax.fori_loop(0, group, gather, jnp.zeros((modes, width), F32))
            entries[g] = entering

            @pl.when(group > 0)
            def _():
                share_copy(g).start()

            entry[...] = reach * entering + jnp.where(odd == 1, other[g], 0.0)

        @pl.when(jnp.logical_not(own))
        def _():
            @pl.when(group > 0)
            def _():
                share_copy(g).wait_recv()

            @pl.when(odd == 1)
            def _():
                pair_copy(g).wait_recv()

            entry[...] = reach * shared[g] + jnp.where(odd == 1, other[g], 0.0)

        for k in range(cells):
            enter(g, k)

        def one(k, inner):
            output(g, k)
            return inner

        lax.fori_loop(0, cells, one, 0)
        return carry

    lax.fori_loop(0, chunks, finish, 0)
    w_load.wait()
    for c in range(chans // LANES):
        gated[:, c * LANES : (c + 1) * LANES] = natural[c].astype(BF16)
    rows_in = gated[...]
    for a in range(0, out_ref.shape[1], 2 * LANES):
        piece = jnp.dot(rows_in, w_in[:, a : a + 2 * LANES], preferred_element_type=F32)
        out_ref[:, a : a + 2 * LANES] = piece.astype(out_ref.dtype)

    @pl.when(me < n - 1)
    def _():
        tail_copy().wait_send()

    for g in range(chunks):
        kept = 2 * g // chunks

        @pl.when(jnp.logical_or(odd == 0, odd != kept))
        def _():
            pair_copy(g).wait_send()

        @pl.when(odd == kept)
        def _():
            def sent(target, carry):
                group_copy(group, target, g).wait_send()
                return carry

            lax.fori_loop(group + 1, groups, sent, 0)

    @pl.when(group > 0)
    def _():
        for g in range(chunks):
            @pl.when(odd == 2 * g // chunks)
            def _():
                share_copy(g).wait_send()


def solution(mesh):
    n = mesh.shape["seq"]

    def body(queries, keys, values, short_taps, decay, residue, skip, w_out):
        rows, chans = queries.shape
        modes = decay.shape[1]
        width = math.gcd(chans, 512)
        chunks = chans // width
        steps = rows // SUB
        hbm = pl.BlockSpec(memory_space=pl.ANY)
        dma = pltpu.SemaphoreType.DMA
        table = pltpu.VMEM((modes, chans), F32)
        tokens = pltpu.VMEM((rows, chans), BF16)
        placed = pltpu.VMEM((steps, SUB, chans), F32)
        operands = (queries, keys, values, short_taps, decay.T, residue.T, skip[None, :], w_out)
        return pl.pallas_call(
            functools.partial(kernel, n, width),
            out_shape=pltpu.VMEM((rows, w_out.shape[1]), BF16),
            in_specs=[hbm] * 8,
            out_specs=pl.BlockSpec(memory_space=pltpu.VMEM),
            scratch_shapes=[
                tokens, tokens, tokens,
                pltpu.VMEM(short_taps.shape, F32),
                table, table,
                pltpu.VMEM((1, chans), F32),
                pltpu.VMEM(w_out.shape, BF16),
                pltpu.VMEM((SUB, chans), BF16),
                pltpu.VMEM((SUB, chans), BF16),
                pltpu.VMEM((SUB, chans), F32),
                pltpu.VMEM(((steps + 2) * SUB, rows), BF16),
                pltpu.VMEM((3, (steps + 2) * SUB, min(width, 2 * LANES)), F32),
                pltpu.VMEM((2, (steps + 2) * SUB, min(width, 2 * LANES)), F32),
                table, table, table, table, table,
                pltpu.VMEM((2, steps, LANES), F32),
                pltpu.VMEM((4, SUB, chans), F32),
                placed, placed, placed,
                pltpu.VMEM((modes * SUB, chans), F32),
                pltpu.VMEM((SUB, modes, chans), F32),
                pltpu.VMEM((width // LANES, modes * SUB, LANES), F32),
                pltpu.VMEM((width // LANES, modes * SUB, LANES), F32),
                pltpu.VMEM((chans // LANES, rows, LANES), F32),
                tokens,
                pltpu.VMEM((modes, width), F32),
                pltpu.VMEM((chunks, modes, width), F32),
                pltpu.VMEM((chunks, modes, width), F32),
                pltpu.VMEM((chunks, modes, width), F32),
                pltpu.VMEM((chunks, modes, width), F32),
                pltpu.VMEM((chunks, modes, width), BF16),
                pltpu.VMEM((n // 2, chunks, modes, width), BF16),
                dma((7,)),
                dma,
                dma((2,)),
                dma((chunks,)),
                dma((chunks,)),
                dma((n // 2, chunks)),
                dma((n // 2, chunks)),
                dma((chunks,)),
                dma((chunks,)),
                pltpu.SemaphoreType.REGULAR((n // 2,)),
            ],
            compiler_params=pltpu.CompilerParams(
                collective_id=0, has_side_effects=True, vmem_limit_bytes=44 * 1024 * 1024
            ),
        )(*(pltpu.with_memory_space_constraint(x, pltpu.HBM) for x in operands))

    placed = (P(("rep", "seq"), None),) * 3 + (P(),) * 5
    return jax.shard_map(
        body, mesh=mesh, in_specs=placed, out_specs=P(("rep", "seq"), None), check_vma=False
    )
```

```python
import functools
import math

import jax
import jax.numpy as jnp
from jax import lax
from jax.experimental import pallas as pl
from jax.experimental.pallas import tpu as pltpu
from jax.sharding import PartitionSpec as P

MESH = pl.DeviceIdType.MESH
F32 = jnp.float32
BF16 = jnp.bfloat16
SUB = 8
LANES = 128


def kernel(
    n, width,
    q_hbm, k_hbm, v_hbm, taps_hbm, rates_hbm, residue_hbm, skip_hbm, w_hbm,
    out_ref,
    q_in, k_in, v_in, taps_ref, rates_ref, residue_ref, skip_ref, w_in,
    tails_out, tails_in, tails, order, moved, fresh, fade_ref, skip2_ref, stride_ref, span_ref, weight_ref,
    filter_ref, edge, sig, q_short, partial, local, segments, turn, work, natural,
    gated, entry, entries, shared, ends, other, totals, earlier,
    in_sems, w_sem, tail_sems, pair_send, pair_recv, group_send, group_recv, share_send, share_recv, credits,
):
    rows, chans = q_in.shape
    modes = rates_ref.shape[0]
    steps = rows // SUB
    chunks = chans // width
    cells = width // LANES
    groups = n // 2
    me = lax.axis_index("seq")
    group = lax.div(me, 2)
    odd = lax.rem(me, 2)
    zero = lax.div(me, n)

    barrier = pltpu.get_barrier_semaphore()

    def greet(device):
        pl.semaphore_signal(barrier, inc=1, device_id={"seq": device}, device_id_type=MESH)

    @pl.when(me > 0)
    def _():
        greet(me - 1)

    def later(target, carry):
        greet(2 * target + odd)
        return carry

    lax.fori_loop(group + 1, groups, later, 0)

    loads = [
        pltpu.make_async_copy(src, dst, in_sems.at[i])
        for i, (src, dst) in enumerate((
            (rates_hbm, rates_ref), (k_hbm, k_in), (v_hbm, v_in), (taps_hbm, taps_ref),
            (residue_hbm, residue_ref), (q_hbm, q_in), (skip_hbm, skip_ref),
        ))
    ]
    for load in loads:
        load.start()
    w_load = pltpu.make_async_copy(w_hbm, w_in, w_sem)

    def tail_copy():
        return pltpu.make_async_remote_copy(
            src_ref=tails_out, dst_ref=tails_in, send_sem=tail_sems.at[0], recv_sem=tail_sems.at[1],
            device_id={"seq": lax.rem(me + 1, n)}, device_id_type=MESH,
        )

    def pair_copy(g):
        return pltpu.make_async_remote_copy(
            src_ref=ends.at[g], dst_ref=other.at[g], send_sem=pair_send.at[g], recv_sem=pair_recv.at[g],
            device_id={"seq": me + 1 - 2 * odd}, device_id_type=MESH,
        )

    def keeper(g):
        return lax.div(2 * g, chunks)

    def group_copy(source, target, g):
        return pltpu.make_async_remote_copy(
            src_ref=totals.at[g], dst_ref=earlier.at[source, g],
            send_sem=group_send.at[target, g], recv_sem=group_recv.at[source, g],
            device_id={"seq": 2 * target + odd}, device_id_type=MESH,
        )

    def share_copy(g):
        return pltpu.make_async_remote_copy(
            src_ref=entries.at[g], dst_ref=shared.at[g], send_sem=share_send.at[g], recv_sem=share_recv.at[g],
            device_id={"seq": me + 1 - 2 * odd}, device_id_type=MESH,
        )

    place = lax.broadcasted_iota(jnp.int32, order.shape, 0)
    token = lax.broadcasted_iota(jnp.int32, order.shape, 1)
    wanted = steps * lax.rem(place, SUB) + lax.div(place, SUB) - 2
    order[...] = jnp.where(token == wanted, 1.0, 0.0).astype(BF16)

    @pl.when(me == 0)
    def _():
        tails_in[...] = jnp.zeros_like(tails_in)

    half = (chunks + 1) // 2

    @pl.when(odd == 0)
    def _():
        for g in range(half, chunks):
            other[g] = jnp.zeros(other.shape[1:], F32)

    @pl.when(group == 0)
    def _():
        shared[...] = jnp.zeros_like(shared)

    lane_row = lax.broadcasted_iota(jnp.int32, (SUB, LANES), 0)
    lane_step = lane_row.astype(F32)

    def columns(c):
        return pl.ds(pl.multiple_of(c * LANES, LANES), LANES)

    def chunk(g):
        return pl.ds(pl.multiple_of(g * width, width), width)

    pl.semaphore_wait(barrier, jnp.where(me < n - 1, 1, 0) + group)

    def credit(source, carry):
        pl.semaphore_signal(
            credits.at[group], inc=1, device_id={"seq": 2 * source + odd}, device_id_type=MESH
        )
        return carry

    lax.fori_loop(0, group, credit, 0)

    loads[0].wait()

    def rates_tables(g, carry):
        cols = chunk(g)
        rates = rates_ref[:, cols]
        fade_ref[:, cols] = jnp.exp(-rates)
        skip2_ref[:, cols] = jnp.exp(-float(steps - 2) * rates)
        stride_ref[:, cols] = jnp.exp(-float(steps) * rates)
        span_ref[:, cols] = jnp.exp(-float(rows) * rates)
        return carry

    lax.fori_loop(0, chunks, rates_tables, 0)

    for load in loads[1:4]:
        load.wait()

    loads[5].wait()
    w_load.start()
    last = [tokens[rows - 16 :, :].astype(F32)[14:16] for tokens in (q_in, k_in, v_in)]
    tails_out[...] = jnp.concatenate(last + [jnp.zeros((2, chans), F32)], axis=0).astype(BF16)

    @pl.when(me < n - 1)
    def _():
        tail_copy().start()

    def short(x, taps, i):
        result = taps[0] * x[SUB * (i + 2) : SUB * (i + 3)]
        result = result + taps[1] * x[SUB * (i + 1) : SUB * (i + 2)]
        return result + taps[2] * x[SUB * i : SUB * (i + 1)]

    def tap_rows(which, cols):
        return [taps_ref[which, j : j + 1, cols] for j in range(3)]

    wide = min(2, cells) * LANES
    strips = chans // wide

    def strip(c):
        return pl.ds(pl.multiple_of(c * wide, wide), wide)

    def arrange(tokens, c):
        return jnp.dot(order[...], tokens[:, strip(c)], preferred_element_type=F32)

    def rounded(x):
        return x.astype(BF16).astype(F32)

    def mix(c, carry):
        following = lax.rem(c + 1, strips)
        moved[:2] = fresh[...]
        fresh[0] = arrange(k_in, following)
        fresh[1] = arrange(v_in, following)
        for half in range(wide // LANES):
            cols = columns(c * (wide // LANES) + half)
            xk = moved.at[0, :, half * LANES : (half + 1) * LANES]
            xv = moved.at[1, :, half * LANES : (half + 1) * LANES]
            k_taps = tap_rows(1, cols)
            v_taps = tap_rows(2, cols)
            for i in range(2):
                edge[i, :, cols] = short(xk, k_taps, i)
                edge[2 + i, :, cols] = short(xv, v_taps, i)
            fades = [fade_ref[m : m + 1, cols] for m in range(modes)]
            state = [None] * modes
            for i in range(2, steps):
                u = rounded(short(xk, k_taps, i) * short(xv, v_taps, i))
                sig[i, :, cols] = u
                for m in range(modes):
                    state[m] = u if i == 2 else state[m] * fades[m] + u
            for m in range(modes):
                local[m * SUB : (m + 1) * SUB, cols] = state[m]
            for m in range(0, modes, 4):
                moved[zero + 2, m // 4 * SUB : (m // 4 + 1) * SUB, :LANES] = state[m + 3]
        return carry

    opening = (1 - odd) * half * (strips // chunks)
    fresh[0] = arrange(k_in, opening)
    fresh[1] = arrange(v_in, opening)
    loads[4].wait()
    loads[6].wait()

    def residue_tables(g, carry):
        cols = chunk(g)
        weight_ref[:, cols] = residue_ref[:, cols] * jnp.sqrt(1.0 - jnp.exp(-2.0 * rates_ref[:, cols]))
        return carry

    lax.fori_loop(0, chunks, residue_tables, 0)

    head = lane_row == 0

    def ends_of(which, cols, zeroth, first):
        taps = tap_rows(which, cols)
        one, two = (
            jnp.where(head, tails[2 * which + a : 2 * which + a + 1, cols], 0.0) for a in (1, 0)
        )
        return zeroth + taps[1] * one + taps[2] * two, first + taps[2] * one

    def summarize(c, g, half):
        cols = columns(c)
        k0, k1 = ends_of(1, cols, edge[0, :, cols], edge[1, :, cols])
        v0, v1 = ends_of(2, cols, edge[2, :, cols], edge[3, :, cols])
        u0 = rounded(k0 * v0)
        u1 = rounded(k1 * v1)
        sig[0, :, cols] = u0
        sig[1, :, cols] = u1
        for m in range(modes):
            row = slice(m, m + 1)
            start = fade_ref[row, cols] * u0 + u1
            turn[half, m * SUB : (m + 1) * SUB, :] = (
                local[m * SUB : (m + 1) * SUB, cols] + skip2_ref[row, cols] * start
            )
        scale = weight_ref[:, cols] * fade_ref[:, cols]
        stride = stride_ref[:, cols]
        state = None
        for j in range(SUB):
            part = scale * turn[half, pl.ds(j, modes, stride=SUB), :]
            segments[j, :, cols] = part
            state = part if j == 0 else state * stride + part
        ends[g, :, columns(c - g * cells)] = state

    def combine(g):
        pair_copy(g).wait_recv()

        @pl.when(group < groups - 1)
        def _():
            mine, theirs = ends[g], other[g]
            former = jnp.where(odd == 1, theirs, mine)
            latter = jnp.where(odd == 1, mine, theirs)
            totals[g] = (span_ref[:, chunk(g)] * former + latter).astype(totals.dtype)

            def send(target, inner):
                @pl.when(lax.rem(g, half) == 0)
                def _():
                    pl.semaphore_wait(credits.at[target], 1)

                group_copy(group, target, g).start()
                return inner

            lax.fori_loop(group + 1, groups, send, 0)

    early = jnp.logical_or(me == 0, odd == 1)
    share = strips // chunks

    def stage(t, carry):
        mixing = jnp.where(early, lax.rem(t, 2) == 0, t < chunks)
        turn_at = jnp.where(early, lax.div(t, 2), lax.rem(t, chunks))
        g = lax.rem(turn_at + (1 - odd) * half, chunks)
        own = keeper(g) == odd

        @pl.when(mixing)
        def _():
            lax.fori_loop(g * share, (g + 1) * share, mix, 0)

        @pl.when(jnp.logical_not(mixing))
        def _():
            @pl.when(turn_at == 0)
            def _():
                @pl.when(me > 0)
                def _():
                    tail_copy().wait_recv()

                tails[...] = tails_in[...].astype(F32)

            for c in range(cells):
                summarize(g * cells + c, g, c)

            @pl.when(jnp.logical_or(odd == 0, jnp.logical_not(own)))
            def _():
                pair_copy(g).start()

            @pl.when(jnp.logical_and(own, jnp.logical_or(odd == 0, me == 1)))
            def _():
                combine(g)

        return carry

    lax.fori_loop(0, 2 * chunks, stage, 0)

    def direct(c, carry):
        moved[0] = fresh[0]
        fresh[0] = arrange(q_in, jnp.minimum(c + 1, strips - 1))
        for half in range(wide // LANES):
            cols = columns(c * (wide // LANES) + half)
            response = [jnp.zeros((SUB, LANES), F32) for _ in range(steps // SUB)]
            for m in range(modes):
                row = slice(m, m + 1)
                rates = rates_ref[row, cols]
                term = jnp.exp(-rates * lane_step) * weight_ref[row, cols]
                for b in range(steps // SUB):
                    response[b] = response[b] + term
                    if b + 1 < steps // SUB:
                        term = term * jnp.exp(-float(SUB) * rates)
            response[0] = response[0] + jnp.where(lane_row == 0, skip_ref[:, cols], 0.0)
            for b in range(steps // SUB):
                filter_ref[half, b * SUB : (b + 1) * SUB, :] = response[b]
            xq = moved.at[0, :, half * LANES : (half + 1) * LANES]
            q_taps = tap_rows(0, cols)
            q0, q1 = ends_of(0, cols, short(xq, q_taps, 0), short(xq, q_taps, 1))
            taps = [filter_ref[half, i : i + 1, :] for i in range(steps)]
            signal = [sig[i, :, cols] for i in range(steps)]
            for i in range(steps):
                q_short[i, :, cols] = q0 if i == 0 else q1 if i == 1 else short(xq, q_taps, i)
                acc = taps[0] * signal[i]
                for s in range(i):
                    acc = acc + taps[i - s] * signal[s]
                partial[i, :, cols] = acc
        return carry

    fresh[0] = arrange(q_in, 0)
    lead = strips // 4 * jnp.minimum(group, 2)
    lead = jnp.where(jnp.logical_and(odd == 1, me > 1), lead, strips)
    lax.fori_loop(0, lead, direct, 0)

    @pl.when(jnp.logical_and(odd == 1, me > 1))
    def _():
        def each(g, carry):
            combine(g)
            return carry

        lax.fori_loop(half, chunks, each, 0)

    lax.fori_loop(lead, strips, direct, 0)

    def enter(g, k):
        cols = columns(g * cells + k)
        state = entry[:, k * LANES : (k + 1) * LANES]
        stride = stride_ref[:, cols]
        for j in range(SUB):
            work[k, j * modes : (j + 1) * modes, :] = state
            if j + 1 < SUB:
                state = state * stride + segments[j, :, cols]

    def output(g, k):
        cols = columns(g * cells + k)
        flow = [work[k, pl.ds(m, SUB, stride=modes), :] for m in range(modes)]
        fades = [fade_ref[m : m + 1, cols] for m in range(modes)]
        for i in range(steps):
            terms = list(flow)
            while len(terms) > 1:
                terms = [sum(terms[a : a + 2]) for a in range(0, len(terms), 2)]
            long_out = rounded(partial[i, :, cols] + terms[0])
            natural[g * cells + k, pl.ds(i, SUB, stride=steps), :] = q_short[i, :, cols] * long_out
            if i + 1 < steps:
                flow = [flow[m] * fades[m] for m in range(modes)]

    def receive(s, carry):
        g = s + odd * half
        far = span_ref[:, chunk(g)]
        far = far * far

        def gather(source, state):
            group_copy(source, group, g).wait_recv()
            return state * far + earlier[source, g].astype(F32)

        entries[g] = lax.fori_loop(0, group, gather, jnp.zeros((modes, width), F32))

        @pl.when(group > 0)
        def _():
            share_copy(g).start()

        return carry

    lax.fori_loop(0, jnp.where(odd == 1, chunks - half, half), receive, 0)

    def finish(s, carry):
        g = lax.rem(s + odd * half, chunks)
        own = keeper(g) == odd
        reach = jnp.where(odd == 1, span_ref[:, chunk(g)], 1.0)

        @pl.when(jnp.logical_not(own))
        def _():
            @pl.when(group > 0)
            def _():
                share_copy(g).wait_recv()

            @pl.when(odd == 1)
            def _():
                pair_copy(g).wait_recv()

        entering = jnp.where(own, entries[g], shared[g])
        entry[...] = reach * entering + jnp.where(odd == 1, other[g], 0.0)
        for k in range(cells):
            enter(g, k)

        def one(k, inner):
            output(g, k)
            return inner

        lax.fori_loop(0, cells, one, 0)
        return carry

    lax.fori_loop(0, chunks, finish, 0)
    w_load.wait()
    for c in range(chans // LANES):
        gated[:, c * LANES : (c + 1) * LANES] = natural[c].astype(BF16)
    rows_in = gated[...]
    for a in range(0, out_ref.shape[1], 2 * LANES):
        piece = jnp.dot(rows_in, w_in[:, a : a + 2 * LANES], preferred_element_type=F32)
        out_ref[:, a : a + 2 * LANES] = piece.astype(out_ref.dtype)

    @pl.when(me < n - 1)
    def _():
        tail_copy().wait_send()

    for g in range(chunks):
        kept = 2 * g // chunks

        @pl.when(jnp.logical_or(odd == 0, odd != kept))
        def _():
            pair_copy(g).wait_send()

        @pl.when(odd == kept)
        def _():
            def sent(target, carry):
                group_copy(group, target, g).wait_send()
                return carry

            lax.fori_loop(group + 1, groups, sent, 0)

    @pl.when(group > 0)
    def _():
        for g in range(chunks):
            @pl.when(odd == 2 * g // chunks)
            def _():
                share_copy(g).wait_send()


def solution(mesh):
    n = mesh.shape["seq"]

    def body(queries, keys, values, short_taps, decay, residue, skip, w_out):
        rows, chans = queries.shape
        modes = decay.shape[1]
        width = math.gcd(chans, 512)
        chunks = chans // width
        steps = rows // SUB
        hbm = pl.BlockSpec(memory_space=pl.ANY)
        dma = pltpu.SemaphoreType.DMA
        table = pltpu.VMEM((modes, chans), F32)
        tokens = pltpu.VMEM((rows, chans), BF16)
        placed = pltpu.VMEM((steps, SUB, chans), F32)
        operands = (queries, keys, values, short_taps, decay.T, residue.T, skip[None, :], w_out)
        return pl.pallas_call(
            functools.partial(kernel, n, width),
            out_shape=pltpu.VMEM((rows, w_out.shape[1]), BF16),
            in_specs=[hbm] * 8,
            out_specs=pl.BlockSpec(memory_space=pltpu.VMEM),
            scratch_shapes=[
                tokens, tokens, tokens,
                pltpu.VMEM(short_taps.shape, F32),
                table, table,
                pltpu.VMEM((1, chans), F32),
                pltpu.VMEM(w_out.shape, BF16),
                pltpu.VMEM((SUB, chans), BF16),
                pltpu.VMEM((SUB, chans), BF16),
                pltpu.VMEM((SUB, chans), F32),
                pltpu.VMEM(((steps + 2) * SUB, rows), BF16),
                pltpu.VMEM((3, (steps + 2) * SUB, min(width, 2 * LANES)), F32),
                pltpu.VMEM((2, (steps + 2) * SUB, min(width, 2 * LANES)), F32),
                table, table, table, table, table,
                pltpu.VMEM((2, steps, LANES), F32),
                pltpu.VMEM((4, SUB, chans), F32),
                placed, placed, placed,
                pltpu.VMEM((modes * SUB, chans), F32),
                pltpu.VMEM((SUB, modes, chans), F32),
                pltpu.VMEM((width // LANES, modes * SUB, LANES), F32),
                pltpu.VMEM((width // LANES, modes * SUB, LANES), F32),
                pltpu.VMEM((chans // LANES, rows, LANES), F32),
                tokens,
                pltpu.VMEM((modes, width), F32),
                pltpu.VMEM((chunks, modes, width), F32),
                pltpu.VMEM((chunks, modes, width), F32),
                pltpu.VMEM((chunks, modes, width), F32),
                pltpu.VMEM((chunks, modes, width), F32),
                pltpu.VMEM((chunks, modes, width), BF16),
                pltpu.VMEM((n // 2, chunks, modes, width), BF16),
                dma((7,)),
                dma,
                dma((2,)),
                dma((chunks,)),
                dma((chunks,)),
                dma((n // 2, chunks)),
                dma((n // 2, chunks)),
                dma((chunks,)),
                dma((chunks,)),
                pltpu.SemaphoreType.REGULAR((n // 2,)),
            ],
            compiler_params=pltpu.CompilerParams(
                collective_id=0, has_side_effects=True, vmem_limit_bytes=44 * 1024 * 1024
            ),
        )(*(pltpu.with_memory_space_constraint(x, pltpu.HBM) for x in operands))

    placed = (P(("rep", "seq"), None),) * 3 + (P(),) * 5
    return jax.shard_map(
        body, mesh=mesh, in_specs=placed, out_specs=P(("rep", "seq"), None), check_vma=False
    )
```

```python
import functools
import math

import jax
import jax.numpy as jnp
from jax import lax
from jax.experimental import pallas as pl
from jax.experimental.pallas import tpu as pltpu
from jax.sharding import PartitionSpec as P

MESH = pl.DeviceIdType.MESH
F32 = jnp.float32
BF16 = jnp.bfloat16
SUB = 8
LANES = 128


def kernel(
    n, width,
    q_hbm, k_hbm, v_hbm, taps_hbm, rates_hbm, residue_hbm, skip_hbm, w_hbm,
    out_ref,
    q_in, k_in, v_in, taps_ref, rates_ref, residue_ref, skip_ref, w_in,
    tails_out, tails_in, tails, order, moved, fresh, fade_ref, skip2_ref, stride_ref, span_ref, weight_ref,
    filter_ref, edge, sig, q_short, partial, local, segments, turn, work, natural,
    gated, entry, entries, shared, ends, other, totals, earlier,
    in_sems, w_sem, tail_sems, pair_send, pair_recv, group_send, group_recv, share_send, share_recv, credits,
):
    rows, chans = q_in.shape
    modes = rates_ref.shape[0]
    steps = rows // SUB
    chunks = chans // width
    cells = width // LANES
    groups = n // 2
    me = lax.axis_index("seq")
    group = lax.div(me, 2)
    odd = lax.rem(me, 2)
    zero = lax.div(me, n)

    barrier = pltpu.get_barrier_semaphore()

    def greet(device):
        pl.semaphore_signal(barrier, inc=1, device_id={"seq": device}, device_id_type=MESH)

    @pl.when(me > 0)
    def _():
        greet(me - 1)

    def later(target, carry):
        greet(2 * target + odd)
        return carry

    lax.fori_loop(group + 1, groups, later, 0)

    loads = [
        pltpu.make_async_copy(src, dst, in_sems.at[i])
        for i, (src, dst) in enumerate((
            (rates_hbm, rates_ref), (k_hbm, k_in), (v_hbm, v_in), (taps_hbm, taps_ref),
            (residue_hbm, residue_ref), (q_hbm, q_in), (skip_hbm, skip_ref),
        ))
    ]
    for i in (1, 2, 5, 0, 3, 4, 6):
        loads[i].start()
    w_load = pltpu.make_async_copy(w_hbm, w_in, w_sem)

    def tail_copy():
        return pltpu.make_async_remote_copy(
            src_ref=tails_out, dst_ref=tails_in, send_sem=tail_sems.at[0], recv_sem=tail_sems.at[1],
            device_id={"seq": lax.rem(me + 1, n)}, device_id_type=MESH,
        )

    def pair_copy(g):
        return pltpu.make_async_remote_copy(
            src_ref=ends.at[g], dst_ref=other.at[g], send_sem=pair_send.at[g], recv_sem=pair_recv.at[g],
            device_id={"seq": me + 1 - 2 * odd}, device_id_type=MESH,
        )

    def keeper(g):
        return lax.div(2 * g, chunks)

    def group_copy(source, target, g):
        return pltpu.make_async_remote_copy(
            src_ref=totals.at[g], dst_ref=earlier.at[source, g],
            send_sem=group_send.at[target, g], recv_sem=group_recv.at[source, g],
            device_id={"seq": 2 * target + odd}, device_id_type=MESH,
        )

    def share_copy(g):
        return pltpu.make_async_remote_copy(
            src_ref=entries.at[g], dst_ref=shared.at[g], send_sem=share_send.at[g], recv_sem=share_recv.at[g],
            device_id={"seq": me + 1 - 2 * odd}, device_id_type=MESH,
        )

    place = lax.broadcasted_iota(jnp.int32, order.shape, 0)
    token = lax.broadcasted_iota(jnp.int32, order.shape, 1)
    wanted = steps * lax.rem(place, SUB) + lax.div(place, SUB) - 2
    order[...] = jnp.where(token == wanted, 1.0, 0.0).astype(BF16)

    @pl.when(me == 0)
    def _():
        tails_in[...] = jnp.zeros_like(tails_in)

    half = (chunks + 1) // 2

    @pl.when(odd == 0)
    def _():
        for g in range(half, chunks):
            other[g] = jnp.zeros(other.shape[1:], F32)

    @pl.when(group == 0)
    def _():
        shared[...] = jnp.zeros_like(shared)

    lane_row = lax.broadcasted_iota(jnp.int32, (SUB, LANES), 0)
    lane_step = lane_row.astype(F32)

    def columns(c):
        return pl.ds(pl.multiple_of(c * LANES, LANES), LANES)

    def chunk(g):
        return pl.ds(pl.multiple_of(g * width, width), width)

    pl.semaphore_wait(barrier, jnp.where(me < n - 1, 1, 0) + group)

    def credit(source, carry):
        pl.semaphore_signal(
            credits.at[group], inc=1, device_id={"seq": 2 * source + odd}, device_id_type=MESH
        )
        return carry

    lax.fori_loop(0, group, credit, 0)

    loads[0].wait()

    def rates_tables(g, carry):
        cols = chunk(g)
        rates = rates_ref[:, cols]
        fade_ref[:, cols] = jnp.exp(-rates)
        skip2_ref[:, cols] = jnp.exp(-float(steps - 2) * rates)
        stride_ref[:, cols] = jnp.exp(-float(steps) * rates)
        span_ref[:, cols] = jnp.exp(-float(rows) * rates)
        return carry

    lax.fori_loop(0, chunks, rates_tables, 0)

    for load in loads[1:4]:
        load.wait()

    loads[5].wait()
    w_load.start()
    last = [tokens[rows - 16 :, :].astype(F32)[14:16] for tokens in (q_in, k_in, v_in)]
    tails_out[...] = jnp.concatenate(last + [jnp.zeros((2, chans), F32)], axis=0).astype(BF16)

    @pl.when(me < n - 1)
    def _():
        tail_copy().start()

    def short(x, taps, i):
        result = taps[0] * x[SUB * (i + 2) : SUB * (i + 3)]
        result = result + taps[1] * x[SUB * (i + 1) : SUB * (i + 2)]
        return result + taps[2] * x[SUB * i : SUB * (i + 1)]

    def tap_rows(which, cols):
        return [taps_ref[which, j : j + 1, cols] for j in range(3)]

    wide = min(2, cells) * LANES
    strips = chans // wide

    def strip(c):
        return pl.ds(pl.multiple_of(c * wide, wide), wide)

    def arrange(tokens, c):
        return jnp.dot(order[...], tokens[:, strip(c)], preferred_element_type=F32)

    def rounded(x):
        return x.astype(BF16).astype(F32)

    def mix(c, carry):
        following = lax.rem(c + 1, strips)
        moved[:2] = fresh[...]
        fresh[0] = arrange(k_in, following)
        fresh[1] = arrange(v_in, following)
        for half in range(wide // LANES):
            cols = columns(c * (wide // LANES) + half)
            xk = moved.at[0, :, half * LANES : (half + 1) * LANES]
            xv = moved.at[1, :, half * LANES : (half + 1) * LANES]
            k_taps = tap_rows(1, cols)
            v_taps = tap_rows(2, cols)
            for i in range(2):
                edge[i, :, cols] = short(xk, k_taps, i)
                edge[2 + i, :, cols] = short(xv, v_taps, i)
            fades = [fade_ref[m : m + 1, cols] for m in range(modes)]
            state = [None] * modes
            for i in range(2, steps):
                u = rounded(short(xk, k_taps, i) * short(xv, v_taps, i))
                sig[i, :, cols] = u
                for m in range(modes):
                    state[m] = u if i == 2 else state[m] * fades[m] + u
            for m in range(modes):
                local[m * SUB : (m + 1) * SUB, cols] = state[m]
            for m in range(0, modes, 4):
                moved[zero + 2, m // 4 * SUB : (m // 4 + 1) * SUB, :LANES] = state[m + 3]
        return carry

    opening = (1 - odd) * half * (strips // chunks)
    fresh[0] = arrange(k_in, opening)
    fresh[1] = arrange(v_in, opening)
    loads[4].wait()
    loads[6].wait()

    def residue_tables(g, carry):
        cols = chunk(g)
        weight_ref[:, cols] = residue_ref[:, cols] * jnp.sqrt(1.0 - jnp.exp(-2.0 * rates_ref[:, cols]))
        return carry

    lax.fori_loop(0, chunks, residue_tables, 0)

    head = lane_row == 0

    def ends_of(which, cols, zeroth, first):
        taps = tap_rows(which, cols)
        one, two = (
            jnp.where(head, tails[2 * which + a : 2 * which + a + 1, cols], 0.0) for a in (1, 0)
        )
        return zeroth + taps[1] * one + taps[2] * two, first + taps[2] * one

    def summarize(c, g, half):
        cols = columns(c)
        k0, k1 = ends_of(1, cols, edge[0, :, cols], edge[1, :, cols])
        v0, v1 = ends_of(2, cols, edge[2, :, cols], edge[3, :, cols])
        u0 = rounded(k0 * v0)
        u1 = rounded(k1 * v1)
        sig[0, :, cols] = u0
        sig[1, :, cols] = u1
        for m in range(modes):
            row = slice(m, m + 1)
            start = fade_ref[row, cols] * u0 + u1
            turn[half, m * SUB : (m + 1) * SUB, :] = (
                local[m * SUB : (m + 1) * SUB, cols] + skip2_ref[row, cols] * start
            )
        scale = weight_ref[:, cols] * fade_ref[:, cols]
        stride = stride_ref[:, cols]
        state = None
        for j in range(SUB):
            part = scale * turn[half, pl.ds(j, modes, stride=SUB), :]
            segments[j, :, cols] = part
            state = part if j == 0 else state * stride + part
        ends[g, :, columns(c - g * cells)] = state

    def combine(g):
        pair_copy(g).wait_recv()

        @pl.when(group < groups - 1)
        def _():
            mine, theirs = ends[g], other[g]
            former = jnp.where(odd == 1, theirs, mine)
            latter = jnp.where(odd == 1, mine, theirs)
            totals[g] = (span_ref[:, chunk(g)] * former + latter).astype(totals.dtype)

            def send(target, inner):
                @pl.when(lax.rem(g, half) == 0)
                def _():
                    pl.semaphore_wait(credits.at[target], 1)

                group_copy(group, target, g).start()
                return inner

            lax.fori_loop(group + 1, groups, send, 0)

    early = jnp.logical_or(me == 0, odd == 1)
    share = strips // chunks

    def stage(t, carry):
        mixing = jnp.where(early, lax.rem(t, 2) == 0, t < chunks)
        turn_at = jnp.where(early, lax.div(t, 2), lax.rem(t, chunks))
        g = lax.rem(turn_at + (1 - odd) * half, chunks)
        own = keeper(g) == odd

        @pl.when(mixing)
        def _():
            lax.fori_loop(g * share, (g + 1) * share, mix, 0)

        @pl.when(jnp.logical_not(mixing))
        def _():
            @pl.when(turn_at == 0)
            def _():
                @pl.when(me > 0)
                def _():
                    tail_copy().wait_recv()

                tails[...] = tails_in[...].astype(F32)

            for c in range(cells):
                summarize(g * cells + c, g, c)

            @pl.when(jnp.logical_or(odd == 0, jnp.logical_not(own)))
            def _():
                pair_copy(g).start()

            @pl.when(jnp.logical_and(own, jnp.logical_or(odd == 0, me == 1)))
            def _():
                combine(g)

        return carry

    lax.fori_loop(0, 2 * chunks, stage, 0)

    def direct(c, carry):
        moved[0] = fresh[0]
        fresh[0] = arrange(q_in, jnp.minimum(c + 1, strips - 1))
        for half in range(wide // LANES):
            cols = columns(c * (wide // LANES) + half)
            response = [jnp.zeros((SUB, LANES), F32) for _ in range(steps // SUB)]
            for m in range(modes):
                row = slice(m, m + 1)
                rates = rates_ref[row, cols]
                term = jnp.exp(-rates * lane_step) * weight_ref[row, cols]
                for b in range(steps // SUB):
                    response[b] = response[b] + term
                    if b + 1 < steps // SUB:
                        term = term * jnp.exp(-float(SUB) * rates)
            response[0] = response[0] + jnp.where(lane_row == 0, skip_ref[:, cols], 0.0)
            for b in range(steps // SUB):
                filter_ref[half, b * SUB : (b + 1) * SUB, :] = response[b]
            xq = moved.at[0, :, half * LANES : (half + 1) * LANES]
            q_taps = tap_rows(0, cols)
            q0, q1 = ends_of(0, cols, short(xq, q_taps, 0), short(xq, q_taps, 1))
            taps = [filter_ref[half, i : i + 1, :] for i in range(steps)]
            signal = [sig[i, :, cols] for i in range(steps)]
            for i in range(steps):
                q_short[i, :, cols] = q0 if i == 0 else q1 if i == 1 else short(xq, q_taps, i)
                acc = taps[0] * signal[i]
                for s in range(i):
                    acc = acc + taps[i - s] * signal[s]
                partial[i, :, cols] = acc
        return carry

    fresh[0] = arrange(q_in, 0)
    lead = strips // 4 * jnp.minimum(group, 2)
    lead = jnp.where(jnp.logical_and(odd == 1, me > 1), lead, strips)
    lax.fori_loop(0, lead, direct, 0)

    @pl.when(jnp.logical_and(odd == 1, me > 1))
    def _():
        def each(g, carry):
            combine(g)
            return carry

        lax.fori_loop(half, chunks, each, 0)

    lax.fori_loop(lead, strips, direct, 0)

    def enter(g, k):
        cols = columns(g * cells + k)
        state = entry[:, k * LANES : (k + 1) * LANES]
        stride = stride_ref[:, cols]
        for j in range(SUB):
            work[k, j * modes : (j + 1) * modes, :] = state
            if j + 1 < SUB:
                state = state * stride + segments[j, :, cols]

    def output(g, k):
        cols = columns(g * cells + k)
        flow = [work[k, pl.ds(m, SUB, stride=modes), :] for m in range(modes)]
        fades = [fade_ref[m : m + 1, cols] for m in range(modes)]
        for i in range(steps):
            terms = list(flow)
            while len(terms) > 1:
                terms = [sum(terms[a : a + 2]) for a in range(0, len(terms), 2)]
            long_out = rounded(partial[i, :, cols] + terms[0])
            natural[g * cells + k, pl.ds(i, SUB, stride=steps), :] = q_short[i, :, cols] * long_out
            if i + 1 < steps:
                flow = [flow[m] * fades[m] for m in range(modes)]

    def receive(s, carry):
        g = s + odd * half
        far = span_ref[:, chunk(g)]
        far = far * far

        def gather(source, state):
            group_copy(source, group, g).wait_recv()
            return state * far + earlier[source, g].astype(F32)

        entries[g] = lax.fori_loop(0, group, gather, jnp.zeros((modes, width), F32))

        @pl.when(group > 0)
        def _():
            share_copy(g).start()

        return carry

    lax.fori_loop(0, jnp.where(odd == 1, chunks - half, half), receive, 0)

    def finish(s, carry):
        g = lax.rem(s + odd * half, chunks)
        own = keeper(g) == odd
        reach = jnp.where(odd == 1, span_ref[:, chunk(g)], 1.0)

        @pl.when(jnp.logical_not(own))
        def _():
            @pl.when(group > 0)
            def _():
                share_copy(g).wait_recv()

            @pl.when(odd == 1)
            def _():
                pair_copy(g).wait_recv()

        entering = jnp.where(own, entries[g], shared[g])
        entry[...] = reach * entering + jnp.where(odd == 1, other[g], 0.0)
        for k in range(cells):
            enter(g, k)

        def one(k, inner):
            output(g, k)
            return inner

        lax.fori_loop(0, cells, one, 0)
        return carry

    lax.fori_loop(0, chunks, finish, 0)
    w_load.wait()
    for c in range(chans // LANES):
        gated[:, c * LANES : (c + 1) * LANES] = natural[c].astype(BF16)
    rows_in = gated[...]
    for a in range(0, out_ref.shape[1], 2 * LANES):
        piece = jnp.dot(rows_in, w_in[:, a : a + 2 * LANES], preferred_element_type=F32)
        out_ref[:, a : a + 2 * LANES] = piece.astype(out_ref.dtype)

    @pl.when(me < n - 1)
    def _():
        tail_copy().wait_send()

    for g in range(chunks):
        kept = 2 * g // chunks

        @pl.when(jnp.logical_or(odd == 0, odd != kept))
        def _():
            pair_copy(g).wait_send()

        @pl.when(odd == kept)
        def _():
            def sent(target, carry):
                group_copy(group, target, g).wait_send()
                return carry

            lax.fori_loop(group + 1, groups, sent, 0)

    @pl.when(group > 0)
    def _():
        for g in range(chunks):
            @pl.when(odd == 2 * g // chunks)
            def _():
                share_copy(g).wait_send()


def solution(mesh):
    n = mesh.shape["seq"]

    def body(queries, keys, values, short_taps, decay, residue, skip, w_out):
        rows, chans = queries.shape
        modes = decay.shape[1]
        width = math.gcd(chans, 512)
        chunks = chans // width
        steps = rows // SUB
        hbm = pl.BlockSpec(memory_space=pl.ANY)
        dma = pltpu.SemaphoreType.DMA
        table = pltpu.VMEM((modes, chans), F32)
        tokens = pltpu.VMEM((rows, chans), BF16)
        placed = pltpu.VMEM((steps, SUB, chans), F32)
        operands = (queries, keys, values, short_taps, decay.T, residue.T, skip[None, :], w_out)
        return pl.pallas_call(
            functools.partial(kernel, n, width),
            out_shape=pltpu.VMEM((rows, w_out.shape[1]), BF16),
            in_specs=[hbm] * 8,
            out_specs=pl.BlockSpec(memory_space=pltpu.VMEM),
            scratch_shapes=[
                tokens, tokens, tokens,
                pltpu.VMEM(short_taps.shape, F32),
                table, table,
                pltpu.VMEM((1, chans), F32),
                pltpu.VMEM(w_out.shape, BF16),
                pltpu.VMEM((SUB, chans), BF16),
                pltpu.VMEM((SUB, chans), BF16),
                pltpu.VMEM((SUB, chans), F32),
                pltpu.VMEM(((steps + 2) * SUB, rows), BF16),
                pltpu.VMEM((3, (steps + 2) * SUB, min(width, 2 * LANES)), F32),
                pltpu.VMEM((2, (steps + 2) * SUB, min(width, 2 * LANES)), F32),
                table, table, table, table, table,
                pltpu.VMEM((2, steps, LANES), F32),
                pltpu.VMEM((4, SUB, chans), F32),
                placed, placed, placed,
                pltpu.VMEM((modes * SUB, chans), F32),
                pltpu.VMEM((SUB, modes, chans), F32),
                pltpu.VMEM((width // LANES, modes * SUB, LANES), F32),
                pltpu.VMEM((width // LANES, modes * SUB, LANES), F32),
                pltpu.VMEM((chans // LANES, rows, LANES), F32),
                tokens,
                pltpu.VMEM((modes, width), F32),
                pltpu.VMEM((chunks, modes, width), F32),
                pltpu.VMEM((chunks, modes, width), F32),
                pltpu.VMEM((chunks, modes, width), F32),
                pltpu.VMEM((chunks, modes, width), F32),
                pltpu.VMEM((chunks, modes, width), BF16),
                pltpu.VMEM((n // 2, chunks, modes, width), BF16),
                dma((7,)),
                dma,
                dma((2,)),
                dma((chunks,)),
                dma((chunks,)),
                dma((n // 2, chunks)),
                dma((n // 2, chunks)),
                dma((chunks,)),
                dma((chunks,)),
                pltpu.SemaphoreType.REGULAR((n // 2,)),
            ],
            compiler_params=pltpu.CompilerParams(
                collective_id=0, has_side_effects=True, vmem_limit_bytes=44 * 1024 * 1024
            ),
        )(*(pltpu.with_memory_space_constraint(x, pltpu.HBM) for x in operands))

    placed = (P(("rep", "seq"), None),) * 3 + (P(),) * 5
    return jax.shard_map(
        body, mesh=mesh, in_specs=placed, out_specs=P(("rep", "seq"), None), check_vma=False
    )
```
